32 devices in a mesh: swath: 8 (over y, x, core), chan: 4 (over z).
Axes of the slice: x: 2, y: 2, z: 4, core: 2. Of those that a mesh axis runs over, the one named last changes fastest.
Arguments:
- innovations: float32 [524288], P(('swath', 'chan')), may hold values from -6 to 6
- obs_precision: float32 [524288], P(('swath', 'chan')), may hold values from 0.25 to 4
- jacobian: bfloat16 [524288, 128], P(('swath', 'chan')), may hold values from -0.5 to 0.5
- predictors: float32 [8, 524288], P(None, ('swath', 'chan')), may hold values from -5 to 5
- obs_column: int32 [524288], P(('swath', 'chan')), may hold values from 0 to 2047, as said below
- obs_channel: int32 [524288], P(('swath', 'chan')), may hold values from 0 to 5119
- obs_count: int32 [8, 4], P('swath', 'chan'), may hold values from 5461 to 16384, as said below
- smoothing: float32 [128], replicated, may hold values from 0.02 to 0.12
- bias_precision: float32 [8, 5120], P(None, 'chan'), may hold values from 1 to 100
Outputs:
- control_state: float32 [256, 256, 128], P('swath', 'chan')
- bias_increment: float32 [8, 5120], P(None, 'chan')
- residual_norms: float32 [3], replicated
The draws below stay inside these ranges and needn't reach their ends.
Inputs may be any that keep to these rules, and one draw needn't show every extreme that they name: `obs_column`: Row-major index latitude row * 64 + longitude column within the tile of the device that holds the slot; all slots of an aligned block of 128 slots lie in one latitude row. `obs_channel`: channel c belongs to block c // 256, whose coefficients are owned by chan index c // 1280. `obs_count`: slots below the count hold live observations, the rest are ignored; some device is full in every draw.
All inputs are finite; a program needn't handle non-finite values.
Results may differ from the reference program's by a relative error of at most 0.0003.
Values sent between devices are 32-bit elements; how exact they have to be, the bound alone decides.
A program may use at most 128 MiB of HBM per device.

```python
import math
import jax
import jax.numpy as jnp
from jax import lax

LEV = 128
NPRED = 8
OBS_BLOCK = 128
LAT_DEV = 32
LON_DEV = 64
OBS_DEV = 16384
ITERS = 2
OBS_ALL = 524288
CHANNELS = 5120
N_SWATH = 8
N_CHAN = 4


def draw_obs_count(key, part):
    devices_all = N_SWATH * N_CHAN
    counts = jax.random.randint(jax.random.fold_in(key, 11), (devices_all,), OBS_DEV // 3, OBS_DEV + 1)
    fullest = jax.random.randint(jax.random.fold_in(key, 12), (), 0, devices_all)
    counts = jnp.where(jnp.arange(devices_all) == fullest, OBS_DEV, counts)
    return counts.reshape(N_SWATH, N_CHAN).astype(jnp.int32)


def draw_obs_column(key, part):
    block_count = OBS_DEV * N_SWATH * N_CHAN // OBS_BLOCK
    line_rows = jax.random.randint(jax.random.fold_in(key, 21), (block_count,), 0, LAT_DEV)
    line_cols = jax.random.randint(jax.random.fold_in(key, 22), (block_count, OBS_BLOCK), 0, LON_DEV)
    return (line_rows[:, None] * LON_DEV + line_cols).reshape(-1).astype(jnp.int32)


def touch_ends(entries, rng, smallest, largest):
    longest = entries.shape.index(max(entries.shape))
    spots = []
    for shift in (0, 1):
        where = [jax.random.randint(jax.random.fold_in(rng, axis), (), 0, length) for axis, length in enumerate(entries.shape)]
        where[longest] = (where[longest] + shift) % entries.shape[longest]
        spots.append(tuple(where))
    return entries.at[spots[0]].set(smallest).at[spots[1]].set(largest)


def steps_of(own_key, dims, split, least, top_value):
    def one(axis_at, blocks):
        draws = jax.random.uniform(jax.random.fold_in(jax.random.fold_in(own_key, 6), axis_at), (blocks,), jnp.float32, least / len(split), top_value / len(split))
        return jnp.repeat(jnp.exp(draws), dims[axis_at] // blocks).reshape((-1,) + (1,) * (len(dims) - axis_at - 1))

    level = one(*split[0])
    for cut in split[1:]:
        level = level * one(*cut)
    return level


def centred(own_key, shape, deviation, most, pieces=(), kind=jnp.bfloat16):
    result = jax.random.normal(own_key, shape, jnp.float32) * deviation
    if len(pieces) > 0:
        result = steps_of(own_key, shape, pieces, -0.22, 0.18) * result
    return jnp.clip(result, min=-most, max=most).astype(kind)


def setup_inputs(seed: int = 0) -> dict:
    arg_keys = jax.random.split(jax.random.key(seed), 10)
    innovations = centred(arg_keys[0], (OBS_ALL,), 1.0, 6.0, ((0, 32),), jnp.float32)
    obs_precision = jnp.clip(jnp.exp(math.log(4.0) - 2.7725887 * jax.random.uniform(arg_keys[1], (OBS_ALL,), jnp.float32) ** steps_of(arg_keys[1], (OBS_ALL,), ((0, 32),), -0.2, 0.2)), 0.25, 4.0)
    jacobian = centred(arg_keys[2], (OBS_ALL, LEV), LEV ** -0.5, 0.5, ((0, 32),))
    predictors = centred(arg_keys[3], (NPRED, OBS_ALL), 1.0, 5.0, ((1, 32),), jnp.float32)
    obs_column = draw_obs_column(jax.random.fold_in(arg_keys[9], 71), 0)
    obs_channel = touch_ends(jax.random.randint(arg_keys[5], (OBS_ALL,), 0, CHANNELS), jax.random.fold_in(arg_keys[5], 1), 0, CHANNELS - 1).astype(jnp.int32)
    obs_count = draw_obs_count(jax.random.fold_in(arg_keys[9], 71), 0)
    smoothing = jnp.clip(jnp.exp(jax.random.uniform(arg_keys[7], (LEV,), jnp.float32, math.log(0.02), math.log(0.12))), 0.02, 0.12)
    bias_precision = jnp.clip(jnp.exp(math.log(100.0) - 4.6051702 * jax.random.uniform(arg_keys[8], (NPRED, CHANNELS), jnp.float32) ** steps_of(arg_keys[8], (NPRED, CHANNELS), ((1, 4),), -0.2, 0.2)), 1.0, 100.0)
    return dict(innovations=innovations, obs_precision=obs_precision, jacobian=jacobian, predictors=predictors, obs_column=obs_column, obs_channel=obs_channel, obs_count=obs_count, smoothing=smoothing, bias_precision=bias_precision)


def smooth_field(state_field, smoothing):
    padded = jnp.pad(state_field, ((1, 1), (0, 0), (0, 0)))
    beside = padded[:-2] + padded[2:] + jnp.roll(state_field, 1, axis=1) + jnp.roll(state_field, -1, axis=1)
    return state_field + smoothing * (beside - 4.0 * state_field)

def reference(innovations, obs_precision, jacobian, predictors, obs_column, obs_channel, obs_count, smoothing, bias_precision):
    devices_all = N_SWATH * N_CHAN
    lat_all = LAT_DEV * N_SWATH
    lon_all = LON_DEV * N_CHAN
    cells_all = lat_all * lon_all
    slot_ids = jnp.arange(devices_all * OBS_DEV, dtype=jnp.int32)
    holder = slot_ids // OBS_DEV
    row_index = holder // N_CHAN * LAT_DEV + obs_column // LON_DEV
    col_index = holder % N_CHAN * LON_DEV + obs_column % LON_DEV
    flat_cell = (row_index * lon_all + col_index).astype(jnp.int32)
    live = slot_ids % OBS_DEV < obs_count.reshape(-1)[holder]
    weights = jnp.where(live, obs_precision, jnp.zeros_like(obs_precision))
    jac_blocks = jacobian.reshape(devices_all, OBS_DEV, LEV)
    cell_blocks = flat_cell.reshape(devices_all, OBS_DEV)

    def forward(state_field):
        table = state_field.reshape(cells_all, LEV)

        def one_block(pair):
            return lax.optimization_barrier(jnp.sum(pair[0].astype(jnp.float32) * table[pair[1]], axis=1))
        return lax.map(one_block, (jac_blocks, cell_blocks)).reshape(-1)

    def adjoint(values):
        value_blocks = values.reshape(devices_all, OBS_DEV)

        def add_block(table, triple):
            return (table.at[triple[1]].add(triple[0].astype(jnp.float32) * triple[2][:, None]), 0)
        start_table = jnp.zeros((cells_all, LEV), jnp.float32)
        table = lax.scan(add_block, start_table, (jac_blocks, cell_blocks, value_blocks))[0]
        return table.reshape(lat_all, lon_all, LEV)

    def bias_forward(coefs):
        return lax.optimization_barrier(jnp.sum(predictors * coefs[:, obs_channel], axis=0))

    def bias_adjoint(terms):
        return jnp.zeros((NPRED, CHANNELS), jnp.float32).at[:, obs_channel].add(terms)

    def hessian(state_dir, bias_dir):
        image = weights * (forward(smooth_field(state_dir, smoothing)) + bias_forward(bias_dir))
        return (state_dir + smooth_field(adjoint(image), smoothing), bias_precision * bias_dir + bias_adjoint(predictors * image[None, :]))
    source = weights * innovations
    res_state = smooth_field(adjoint(source), smoothing)
    res_bias = bias_adjoint(predictors * source[None, :])
    diagonal = bias_precision + bias_adjoint(predictors * predictors * weights[None, :])
    sol_state = jnp.zeros_like(res_state)
    sol_bias = jnp.zeros_like(res_bias)
    pre_bias = res_bias / diagonal
    dir_state, dir_bias = (res_state, pre_bias)
    state_sq = jnp.sum(res_state * res_state)
    rz_now = state_sq + jnp.sum(res_bias * pre_bias)
    record = [state_sq + jnp.sum(res_bias * res_bias)]
    for turn_index in range(ITERS):
        img_state, img_bias = hessian(dir_state, dir_bias)
        length = rz_now / (jnp.sum(dir_state * img_state) + jnp.sum(dir_bias * img_bias))
        sol_state = sol_state + length * dir_state
        sol_bias = sol_bias + length * dir_bias
        res_state = res_state - length * img_state
        res_bias = res_bias - length * img_bias
        pre_bias = res_bias / diagonal
        state_sq = jnp.sum(res_state * res_state)
        rz_next = state_sq + jnp.sum(res_bias * pre_bias)
        record.append(state_sq + jnp.sum(res_bias * res_bias))
        ratio = rz_next / rz_now
        dir_state = res_state + ratio * dir_state
        dir_bias = pre_bias + ratio * dir_bias
        rz_now = rz_next
    return (sol_state, sol_bias, jnp.sqrt(jnp.stack(record)))
```

```python
import functools

import jax
import jax.numpy as jnp
from jax import lax
from jax.experimental import pallas as pl
from jax.experimental.pallas import tpu as pltpu
from jax.sharding import PartitionSpec as P

LEV = 128
NPRED = 8
CH_BLOCK = 256
OBS_BLOCK = 128
LAT_DEV = 32
LON_DEV = 64
ITERS = 2
LINES = 8
PAIRS = LINES // 2
PAIR = 2 * OBS_BLOCK
LANES = 128
TILE = (8, LANES)
F32 = jnp.float32
BF16 = jnp.bfloat16
NT = (((1,), (1,)), ((), ()))
VMEM_LIMIT = 60 * 1024 * 1024


def halves(value):
    high = value.astype(BF16)
    return high, (value - high.astype(F32)).astype(BF16)


def fold(value):
    total = value[0:8]
    for i in range(1, value.shape[0] // 8):
        total = total + value[8 * i : 8 * i + 8]
    return total


def total_of(parts):
    total = parts[0]
    for part in parts[1:]:
        total = total + part
    return total


def kernel(n, m, own, blocks, lines, chunk, *refs):
    refs = list(refs)
    take = lambda k: [refs.pop(0) for _ in range(k)]
    count_ref, smooth_ref, bprec_ref = take(3)
    cell_h, chan_h, prec_h, innov_h, pred_h, jac_h = take(6)
    x_out, bias_out, norms_out = take(3)
    cell_ref, chan_ref, prec_ref, innov_ref, pred_ref, jac_ref = take(6)
    hot_ref, msk_ref, w_ref, y_ref, f_ref, part_ref = take(6)
    index_v, index_s = take(2)
    g_ref, gc_ref, r0_ref, r1_ref, p1_ref, rc_ref, split_ref = take(7)
    acc_ref, table_ref, coef_ref = take(3)
    bp_c, diag_c, r_c, p_c, own_all = take(5)
    hu, hd, hc, ta, bb, tf, sz, sw = take(8)
    in_s, ix_s, o_s, o_r, h_s, h_r, ta_s, ta_r, b_s, b_r, c_s, c_r, z_s, z_r, w_s, w_r = take(16)
    width = own * m
    groups = lines // LINES
    me = lax.axis_index("swath")
    z = lax.axis_index("chan")
    per = CH_BLOCK // LANES

    def to_lat(d):
        return {"swath": lax.rem(me + d, n)}

    def to_lon(d):
        return {"chan": lax.rem(z + d, m)}

    pending = []

    def send(src, dst, ss, rs, dev):
        copy = pltpu.make_async_remote_copy(
            src_ref=src, dst_ref=dst, send_sem=ss, recv_sem=rs,
            device_id=dev, device_id_type=pl.DeviceIdType.MESH,
        )
        copy.start()
        pending.append(copy)
        return copy

    def landed(copies):
        for copy in copies:
            copy.wait_recv()

    barrier = pltpu.get_barrier_semaphore()
    for d in range(1, n):
        pl.semaphore_signal(barrier, inc=1, device_id=to_lat(d), device_id_type=pl.DeviceIdType.MESH)
    for d in range(1, m):
        pl.semaphore_signal(barrier, inc=1, device_id=to_lon(d), device_id_type=pl.DeviceIdType.MESH)

    loads = []
    for k, (src, dst) in enumerate((
        (chan_h, chan_ref), (prec_h, prec_ref), (pred_h, pred_ref),
        (innov_h, innov_ref), (cell_h, cell_ref), (jac_h, jac_ref),
    )):
        copy = pltpu.make_async_copy(src, dst, in_s.at[k])
        copy.start()
        loads.append(copy)
    load_chan, load_prec, load_pred, load_innov, load_cell, load_jac = loads

    count = count_ref[0, 0]
    sub = lax.broadcasted_iota(jnp.int32, TILE, 0)
    slot8 = sub * OBS_BLOCK + lax.broadcasted_iota(jnp.int32, TILE, 1)

    def pairs_of(tile):
        return [
            jnp.concatenate([tile[2 * p : 2 * p + 1], tile[2 * p + 1 : 2 * p + 2]], axis=1)
            for p in range(PAIRS)
        ]

    def stack_left(term, mask):
        high = term.astype(BF16).astype(F32)
        low = term - high
        sides = []
        for side in (high, low):
            twice = jnp.concatenate([side, side], axis=0).astype(BF16)
            sides.append(jnp.concatenate([twice] * (blocks // 2), axis=0) * mask)
        return jnp.concatenate(sides, axis=0)

    def add_table(lefts, hots):
        acc_ref[...] += lax.dot_general(
            jnp.concatenate(lefts, axis=1), jnp.concatenate(hots, axis=1), NT,
            preferred_element_type=F32,
        )

    def preds_of(it, p):
        start = pl.multiple_of((it * PAIRS + p) * PAIR, PAIR)
        return pred_ref[:, pl.ds(start, PAIR)]

    def write_table(s):
        half = NPRED * blocks
        for j in range(n * chunk):
            if j < width:
                top = (j // per) * NPRED
                lanes = slice((j % per) * LANES, (j % per + 1) * LANES)
                tile = acc_ref[top : top + NPRED, lanes] + acc_ref[half + top : half + top + NPRED, lanes]
            else:
                tile = jnp.zeros((NPRED, LANES), F32)
            table_ref[s, j // chunk, j % chunk] = tile

    def scatter(s):
        return [
            send(table_ref.at[s, lax.rem(me + d, n)], ta.at[s, d], ta_s.at[s, d], ta_r.at[s, d], to_lat(d))
            for d in range(1, n)
        ]

    def across(s, copies):
        landed(copies)
        bb[s, z] = total_of([table_ref[s, me]] + [ta[s, d] for d in range(1, n)])
        return [
            send(bb.at[s, z], bb.at[s, z], b_s.at[s, d], b_r.at[s, d], to_lon(d)) for d in range(1, m)
        ]

    def chunk_sum(s, copies):
        landed(copies)
        return total_of([bb[s, j] for j in range(m)])

    def gather(i, value):
        tf[i, me] = value
        return [
            send(tf.at[i, me], tf.at[i, me], c_s.at[i, d], c_r.at[i, d], to_lat(d)) for d in range(1, n)
        ]

    def lon_tile(e, tile):
        sz[e, z] = tile
        return [send(sz.at[e, z], sz.at[e, z], z_s.at[e, d], z_r.at[e, d], to_lon(d)) for d in range(1, m)]

    def lon_total(e, copies):
        landed(copies)
        return total_of([sz[e, j] for j in range(m)])

    def lat_tile(e, tile):
        sw[e, me] = tile
        return [send(sw.at[e, me], sw.at[e, me], w_s.at[e, d], w_r.at[e, d], to_lat(d)) for d in range(1, n)]

    def lat_total(e, copies):
        landed(copies)
        return jnp.sum(total_of([sw[e, j] for j in range(n)]), axis=1, keepdims=True)

    def rows_tile(*tiles):
        out = jnp.zeros(TILE, F32)
        for k, tile in enumerate(tiles):
            out = jnp.where(sub == k, jnp.sum(tile, axis=0, keepdims=True), out)
        return out

    def halo(k, field, cols):
        return [
            send(field.at[LAT_DEV - 1], hu.at[k], h_s.at[k, 0], h_r.at[k, 0], to_lat(1)),
            send(field.at[0], hd.at[k], h_s.at[k, 1], h_r.at[k, 1], to_lat(n - 1)),
            send(cols.at[1], hc.at[k, 0], h_s.at[k, 2], h_r.at[k, 2], to_lon(1)),
            send(cols.at[0], hc.at[k, 1], h_s.at[k, 3], h_r.at[k, 3], to_lon(m - 1)),
        ]

    load_chan.wait()
    load_prec.wait()
    load_pred.wait()
    load_innov.wait()
    acc_ref[...] = jnp.zeros_like(acc_ref)
    iota_ch = lax.broadcasted_iota(jnp.int32, (CH_BLOCK, PAIR), 0)
    iota_b = lax.broadcasted_iota(jnp.int32, (NPRED * blocks, PAIR), 0) // NPRED

    def square_step(it, carry):
        base = pl.multiple_of(it * LINES, LINES)
        w8 = jnp.where(base * OBS_BLOCK + slot8 < count, prec_ref[pl.ds(base, LINES), :], 0.0)
        w_ref[pl.ds(base, LINES), :] = w8
        y_ref[pl.ds(base, LINES), :] = w8 * innov_ref[pl.ds(base, LINES), :]
        weights = pairs_of(w8)
        chans = pairs_of(chan_ref[pl.ds(base, LINES), :])
        lefts, hots = [], []
        for p in range(PAIRS):
            hot = jnp.where(iota_ch == chans[p] % CH_BLOCK, 1.0, 0.0).astype(BF16)
            mask = jnp.where(iota_b == chans[p] // CH_BLOCK, 1.0, 0.0).astype(BF16)
            hot_ref[it * PAIRS + p] = hot
            msk_ref[it * PAIRS + p] = mask
            preds = preds_of(it, p)
            lefts.append(stack_left(preds * preds * weights[p], mask))
            hots.append(hot)
        add_table(lefts, hots)
        return carry

    lax.fori_loop(0, groups, square_step, 0)
    write_table(0)

    load_cell.wait()
    first = jnp.broadcast_to(cell_ref[:, 0:1], (lines, LANES)) // LON_DEV
    iota_l = lax.broadcasted_iota(jnp.int32, (lines, LANES), 0)
    iota_r = lax.broadcasted_iota(jnp.int32, (lines, LANES), 1)
    turned = jnp.transpose(first)
    before = jnp.where((first == turned) & (iota_l < iota_r), iota_l, -1)
    before = jnp.max(before, axis=0, keepdims=True)
    last = jnp.max(jnp.where(first == iota_r, iota_l, -1), axis=0, keepdims=True)
    index_v[0:1, :] = turned[0:1, :]
    index_v[1:2, :] = jnp.where(before < 0, lines, before)
    index_v[2:3, :] = jnp.where(last < 0, lines, last)
    load_index = pltpu.make_async_copy(index_v, index_s, ix_s.at[0])
    load_index.start()

    pl.semaphore_wait(barrier, n - 1 + m - 1)
    for j in range(own):
        own_all[z, j] = bprec_ref[:, j * LANES : (j + 1) * LANES]
    squares = scatter(0)
    owners = [send(own_all.at[z], own_all.at[z], o_s.at[d], o_r.at[d], to_lon(d)) for d in range(1, m)]

    def adjoint_bias(s):
        acc_ref[...] = jnp.zeros_like(acc_ref)

        def table_step(it, carry):
            base = pl.multiple_of(it * LINES, LINES)
            values = pairs_of(y_ref[pl.ds(base, LINES), :])
            lefts, hots = [], []
            for p in range(PAIRS):
                lefts.append(stack_left(preds_of(it, p) * values[p], msk_ref[it * PAIRS + p]))
                hots.append(hot_ref[it * PAIRS + p])
            add_table(lefts, hots)
            return carry

        lax.fori_loop(0, groups, table_step, 0)
        write_table(s)
        return scatter(s)

    iota_col = lax.broadcasted_iota(jnp.int32, (LON_DEV, OBS_BLOCK), 0)

    def jac_of(line):
        return jac_ref[pl.ds(pl.multiple_of(line * OBS_BLOCK, OBS_BLOCK), OBS_BLOCK), :]

    def adjoint_state(k):
        def line_step(it, carry):
            base = pl.multiple_of(it * LINES, LINES)
            cols = cell_ref[pl.ds(base, LINES), :] % LON_DEV
            values = y_ref[pl.ds(base, LINES), :]
            outs = []
            for l in range(LINES):
                high, low = halves(jnp.where(iota_col == cols[l : l + 1, :], values[l : l + 1, :], 0.0))
                jac = jac_of(base + l)
                outs.append(jnp.dot(
                    jnp.concatenate([high, low], axis=1), jnp.concatenate([jac, jac], axis=0),
                    preferred_element_type=F32,
                ))
            for l in range(LINES):
                part_ref[base + l] = outs[l] + part_ref[index_s[1, base + l]]
            return carry

        lax.fori_loop(0, groups, line_step, 0)

        def row_step(i, carry):
            row = part_ref[index_s[2, i]]
            g_ref[k, i] = row
            gc_ref[k, 0, pl.ds(i, 1), :] = row[0:1, :]
            gc_ref[k, 1, pl.ds(i, 1), :] = row[LON_DEV - 1 : LON_DEV, :]
            return carry

        lax.fori_loop(0, LAT_DEV, row_step, 0)
        return halo(2 * k, g_ref.at[k], gc_ref.at[k])

    smooth = smooth_ref[0:1, :]
    top_keep = (me > 0).astype(F32)
    bottom_keep = (me < n - 1).astype(F32)
    column = lax.broadcasted_iota(jnp.int32, (LON_DEV, LEV), 0)
    zero = jnp.zeros((LON_DEV, LEV), F32)

    def sweep(field, k, use, acc):
        up, down, side = hu.at[k], hd.at[k], hc.at[k]

        def stencil(i, above, below):
            mid = field[i]
            left = jnp.where(column == 0, side[0, pl.ds(i, 1), :], pltpu.roll(mid, 1, 0))
            right = jnp.where(
                column == LON_DEV - 1, side[1, pl.ds(i, 1), :], pltpu.roll(mid, LON_DEV - 1, 0)
            )
            return mid + smooth * (above + below + left + right - 4.0 * mid)

        acc = use(0, stencil(0, up[...] * top_keep, field[1]), acc)
        inner = LAT_DEV - 2
        group = next(k for k in (5, 4, 3, 2, 1) if inner % k == 0)

        def rows(it, a):
            for k in range(group):
                i = 1 + it * group + k
                a = use(i, stencil(i, field[i - 1], field[i + 1]), a)
            return a

        acc = lax.fori_loop(0, inner // group, rows, acc)
        end = LAT_DEV - 1
        return use(end, stencil(end, field[end - 1], down[...] * bottom_keep), acc)

    def keep_columns(k, i, row):
        rc_ref[k, 0, pl.ds(i, 1), :] = row[0:1]
        rc_ref[k, 1, pl.ds(i, 1), :] = row[LON_DEV - 1 : LON_DEV]

    def forward_state(field, k, old):
        def use(i, row, acc):
            high, low = halves(row)
            split_ref[i] = jnp.concatenate([high, low], axis=1)
            return acc

        sweep(field, k, use, 0)

        def line_step(it, carry):
            base = pl.multiple_of(it * LINES, LINES)
            cols = cell_ref[pl.ds(base, LINES), :] % LON_DEV
            seen = []
            for l in range(LINES):
                jac = jac_of(base + l)
                both = lax.dot_general(
                    split_ref[index_s[0, base + l]], jnp.concatenate([jac, jac], axis=1), NT,
                    preferred_element_type=F32,
                )
                seen.append(jnp.sum(jnp.where(iota_col == cols[l : l + 1, :], both, 0.0), axis=0, keepdims=True))
            y_ref[pl.ds(base, LINES), :] = jnp.concatenate(seen, axis=0)
            return carry

        lax.fori_loop(0, groups, line_step, 0)

    def forward_bias(i, beta):
        for b in range(blocks):
            for h in range(per):
                j = b * per + h
                high, low = halves(tf[i, j // chunk, j % chunk])
                coef_ref[b * NPRED : (b + 1) * NPRED, h * LANES : (h + 1) * LANES] = high
                coef_ref[b * NPRED : (b + 1) * NPRED, CH_BLOCK + h * LANES : CH_BLOCK + (h + 1) * LANES] = low
        coef2 = coef_ref[...]

        def look_step(it, acc):
            base = pl.multiple_of(it * LINES, LINES)
            chans = pairs_of(chan_ref[pl.ds(base, LINES), :])
            looked = []
            for p in range(PAIRS):
                hot = hot_ref[it * PAIRS + p]
                mid = jnp.dot(coef2, jnp.concatenate([hot, hot], axis=0), preferred_element_type=F32)
                which = jnp.broadcast_to(chans[p] // CH_BLOCK, (NPRED, PAIR))
                total = jnp.zeros((NPRED, PAIR), F32)
                for b in range(blocks):
                    total = total + jnp.where(which == b, mid[b * NPRED : (b + 1) * NPRED], 0.0)
                total = jnp.sum(total * preds_of(it, p), axis=0, keepdims=True)
                looked += [total[:, :OBS_BLOCK], total[:, OBS_BLOCK:]]
            f8 = y_ref[pl.ds(base, LINES), :] + jnp.concatenate(looked, axis=0)
            if beta is not None:
                f8 = f8 + beta * f_ref[pl.ds(base, LINES), :]
            y8 = w_ref[pl.ds(base, LINES), :] * f8
            f_ref[pl.ds(base, LINES), :] = f8
            y_ref[pl.ds(base, LINES), :] = y8
            return acc + y8 * f8

        return lax.fori_loop(0, groups, look_step, jnp.zeros(TILE, F32))

    def spread(column):
        return jnp.broadcast_to(column, TILE)

    def dots(*pairs):
        return [total_of([a[j] * b[j] for j in range(chunk)]) for a, b in pairs]

    part_ref[lines] = zero
    sums = adjoint_bias(1)
    squares = across(0, squares)
    load_index.wait()
    load_jac.wait()
    halos = adjoint_state(0)
    sums = across(1, sums)
    landed(halos)

    def use_first(i, row, acc):
        r0_ref[i] = row
        keep_columns(0, i, row)
        return acc + row * row

    pp_state = fold(sweep(g_ref.at[0], 0, use_first, zero))
    halos = halo(1, r0_ref, rc_ref.at[0])
    crossing = lon_tile(0, pp_state)
    landed(owners)
    for j in range(chunk):
        spot = jnp.minimum(me * chunk + j, width - 1)
        bp_c[j] = own_all[spot // own, lax.rem(spot, own)]
    diag_c[...] = bp_c[...] + chunk_sum(0, squares)
    r_c[...] = chunk_sum(1, sums)
    p_c[...] = r_c[...] / diag_c[...]
    gathers = gather(0, p_c[...])
    around = lat_tile(0, rows_tile(lon_total(0, crossing), *dots((r_c, p_c), (r_c, r_c))))
    landed(halos)
    forward_state(r0_ref, 1, None)
    landed(gathers)
    totals = lat_total(0, around)
    rz = spread(totals[0:1] + totals[1:2])
    norms = [spread(totals[0:1] + totals[2:3])]
    beta = None
    alphas = []
    for turn in range(ITERS):
        final = turn == ITERS - 1
        observed = forward_bias(turn, None if beta is None else beta[0:1])
        sums = adjoint_bias(2 + turn)
        if turn > 0:
            slope = beta[0:1]

            def p_step(it, acc):
                for k in range(4):
                    i = it * 4 + k
                    row = r1_ref[i] + slope * r0_ref[i]
                    p1_ref[i] = row
                    acc = acc + row * row
                return acc

            pp_state = fold(lax.fori_loop(0, LAT_DEV // 4, p_step, zero))
            p_c[...] = tf[turn, me] + beta * p_c[...]
        crossing = lon_tile(1 + 2 * turn, pp_state + observed)
        halos = adjoint_state(1 + turn)
        pp_bias = total_of([bp_c[j] * p_c[j] * p_c[j] for j in range(chunk)])
        around = lat_tile(1 + 2 * turn, rows_tile(lon_total(1 + 2 * turn, crossing), pp_bias))
        sums = across(2 + turn, sums)
        totals = lat_total(1 + 2 * turn, around)
        alpha = rz / spread(totals[0:1] + totals[1:2])
        alphas.append(alpha)
        line = alpha[0:1]
        landed(halos)
        p_ref, old_ref = (p1_ref, r1_ref) if turn > 0 else (r0_ref, r0_ref)

        def use_next(i, row, acc):
            new = old_ref[i] - line * (p_ref[i] + row)
            if not final:
                r1_ref[i] = new
                keep_columns(1, i, new)
            return acc + new * new

        rr_state = fold(sweep(g_ref.at[1 + turn], 2 + 2 * turn, use_next, zero))
        crossing = lon_tile(2 + 2 * turn, rr_state)
        if not final:
            halos = halo(3 + 2 * turn, r1_ref, rc_ref.at[1])
        image = bp_c[...] * p_c[...] + chunk_sum(2 + turn, sums)
        r_c[...] = r_c[...] - alpha * image
        z_c = r_c[...] / diag_c[...]
        if not final:
            gathers = gather(turn + 1, z_c)
        around = lat_tile(
            2 + 2 * turn, rows_tile(lon_total(2 + 2 * turn, crossing), *dots((r_c, z_c), (r_c, r_c)))
        )
        if not final:
            landed(halos)
            forward_state(r1_ref, 3 + 2 * turn, None)
            landed(gathers)
        else:
            first_line, last_line = alphas[0][0:1], alphas[1][0:1]

            def x_step(it, carry):
                for k in range(4):
                    i = it * 4 + k
                    x_out[i] = first_line * r0_ref[i] + last_line * p1_ref[i]
                return carry

            lax.fori_loop(0, LAT_DEV // 4, x_step, 0)
            for j in range(own):
                spot = z * own + j
                row, col = spot // chunk, lax.rem(spot, chunk)
                start = tf[0, row, col]
                bias_out[:, j * LANES : (j + 1) * LANES] = alphas[0] * start + alphas[1] * (
                    tf[1, row, col] + beta * start
                )
        totals = lat_total(2 + 2 * turn, around)
        new = spread(totals[0:1] + totals[1:2])
        norms.append(spread(totals[0:1] + totals[2:3]))
        beta = new / rz
        rz = new
    lane = lax.broadcasted_iota(jnp.int32, TILE, 1)
    squares = jnp.zeros(TILE, F32)
    for j in range(ITERS + 1):
        squares = jnp.where(lane == j, norms[j], squares)
    norms_out[...] = jnp.sqrt(squares)
    for copy in pending:
        copy.wait_send()


def shaped(*shape):
    return jax.ShapeDtypeStruct(shape, F32)


def body(
    innovations,
    obs_precision,
    jacobian,
    predictors,
    obs_column,
    obs_channel,
    obs_count,
    smoothing,
    bias_precision,
):
    n = lax.axis_size("swath")
    m = lax.axis_size("chan")
    owned_width = bias_precision.shape[1]
    own = owned_width // LANES
    width = own * m
    blocks = owned_width * m // CH_BLOCK
    slots = obs_precision.shape[0]
    lines = slots // OBS_BLOCK
    chunk = -(-width // n)
    half = NPRED * blocks
    grid_lines = lambda a: a.reshape(lines, OBS_BLOCK)
    vm = lambda *s: pltpu.VMEM(s, F32)
    vb = lambda *s: pltpu.VMEM(s, BF16)
    vi = lambda *s: pltpu.VMEM(s, jnp.int32)
    sem = lambda *s: pltpu.SemaphoreType.DMA(s)
    halos = 1 + 2 * ITERS
    tables = 2 + ITERS
    events = 1 + 2 * ITERS
    scratch = [
        vi(lines, OBS_BLOCK), vi(lines, OBS_BLOCK), vm(lines, OBS_BLOCK), vm(lines, OBS_BLOCK),
        vm(NPRED, slots), vb(slots, LEV),
        vb(lines // 2, CH_BLOCK, PAIR), vb(lines // 2, half, PAIR),
        vm(lines, OBS_BLOCK), vm(lines, OBS_BLOCK), vm(lines, OBS_BLOCK), vm(lines + 1, LON_DEV, LEV),
        vi(8, LANES), pltpu.SMEM((8, LANES), jnp.int32),
        vm(1 + ITERS, LAT_DEV, LON_DEV, LEV), vm(1 + ITERS, 2, LAT_DEV, LEV),
        vm(LAT_DEV, LON_DEV, LEV), vm(LAT_DEV, LON_DEV, LEV), vm(LAT_DEV, LON_DEV, LEV),
        vm(2, 2, LAT_DEV, LEV), vb(LAT_DEV, LON_DEV, 2 * LEV),
        vm(2 * half, CH_BLOCK), vm(tables, n, chunk, NPRED, LANES), vb(half, 2 * CH_BLOCK),
        vm(chunk, NPRED, LANES), vm(chunk, NPRED, LANES), vm(chunk, NPRED, LANES),
        vm(chunk, NPRED, LANES), vm(m, own, NPRED, LANES),
        vm(halos, LON_DEV, LEV), vm(halos, LON_DEV, LEV), vm(halos, 2, LAT_DEV, LEV),
        vm(tables, n, chunk, NPRED, LANES), vm(tables, m, chunk, NPRED, LANES),
        vm(ITERS, n, chunk, NPRED, LANES), vm(events, m, 8, LANES), vm(events, n, 8, LANES),
        sem(6), sem(1), sem(m), sem(m), sem(halos, 4), sem(halos, 4), sem(tables, n), sem(tables, n),
        sem(tables, m), sem(tables, m), sem(ITERS, n), sem(ITERS, n), sem(events, m), sem(events, m),
        sem(events, n), sem(events, n),
    ]
    VM = pl.BlockSpec(memory_space=pltpu.VMEM)
    HB = pl.BlockSpec(memory_space=pltpu.HBM)
    x, bias, norms = pl.pallas_call(
        functools.partial(kernel, n, m, own, blocks, lines, chunk),
        out_shape=(shaped(LAT_DEV, LON_DEV, LEV), shaped(NPRED, owned_width), shaped(8, LANES)),
        in_specs=[pl.BlockSpec(memory_space=pltpu.SMEM), VM, VM] + [HB] * 6,
        out_specs=(VM, VM, VM),
        scratch_shapes=scratch,
        compiler_params=pltpu.CompilerParams(
            collective_id=0, has_side_effects=True, vmem_limit_bytes=VMEM_LIMIT
        ),
        name="cg",
    )(
        obs_count, smoothing.reshape(1, LEV), bias_precision,
        grid_lines(obs_column), grid_lines(obs_channel), grid_lines(obs_precision),
        grid_lines(innovations), predictors, jacobian,
    )
    return (x, bias, norms[0, : ITERS + 1])


def solution(mesh):
    placed = (
        P(("swath", "chan")),
        P(("swath", "chan")),
        P(("swath", "chan"), None),
        P(None, ("swath", "chan")),
        P(("swath", "chan")),
        P(("swath", "chan")),
        P("swath", "chan"),
        P(),
        P(None, "chan"),
    )
    return jax.shard_map(
        body,
        mesh=mesh,
        in_specs=placed,
        out_specs=(P("swath", "chan", None), P(None, "chan"), P()),
        check_vma=False,
    )
```

```python
import functools

import jax
import jax.numpy as jnp
from jax import lax
from jax.experimental import pallas as pl
from jax.experimental.pallas import tpu as pltpu
from jax.sharding import PartitionSpec as P

LEV = 128
NPRED = 8
CH_BLOCK = 256
OBS_BLOCK = 128
LAT_DEV = 32
LON_DEV = 64
ITERS = 2
LINES = 8
PAIRS = LINES // 2
SQUARE_STEP, TABLE_STEP, LOOK_STEP, ADJOINT_STEP, FORWARD_STEP = 2, 4, 4, 4, 4
PAIR = 2 * OBS_BLOCK
LANES = 128
TILE = (8, LANES)
F32 = jnp.float32
BF16 = jnp.bfloat16
NT = (((1,), (1,)), ((), ()))
VMEM_LIMIT = 44 * 1024 * 1024


def halves(value):
    high = value.astype(BF16)
    return high, (value - high.astype(F32)).astype(BF16)


def fold(value):
    total = value[0:8]
    for i in range(1, value.shape[0] // 8):
        total = total + value[8 * i : 8 * i + 8]
    return total


def total_of(parts):
    total = parts[0]
    for part in parts[1:]:
        total = total + part
    return total


def stage(name, run, *args):
    return run(*args)


def kernel(n, m, own, blocks, lines, chunk, *refs):
    refs = list(refs)
    take = lambda k: [refs.pop(0) for _ in range(k)]
    count_ref, smooth_ref, bprec_ref = take(3)
    cell_h, chan_h, prec_h, innov_h, pred_h, jac_h = take(6)
    x_out, bias_out, norms_out = take(3)
    cell_ref, chan_ref, prec_ref, innov_ref, pred_ref, jac_ref = take(6)
    turned_ref, hot_ref, msk_ref, w_ref, y_ref, f_ref, part_ref = take(7)
    index_v, index_s = take(2)
    g_ref, gc_ref, r0_ref, r1_ref, p1_ref, rc_ref, split_ref = take(7)
    acc_ref, table_ref, coef_ref = take(3)
    bp_c, diag_c, r_c, p_c, own_all = take(5)
    hu, hd, hc, ta, bb, tf, sz, sw = take(8)
    in_s, ix_s, o_s, o_r, h_s, h_r, ta_s, ta_r, b_s, b_r, c_s, c_r, z_s, z_r, w_s, w_r = take(16)
    width = own * m
    groups = lines // LINES
    me = lax.axis_index("swath")
    z = lax.axis_index("chan")
    per = CH_BLOCK // LANES

    def to_lat(d):
        return {"swath": lax.rem(me + d, n)}

    def to_lon(d):
        return {"chan": lax.rem(z + d, m)}

    pending = []

    def send(src, dst, ss, rs, dev):
        copy = pltpu.make_async_remote_copy(
            src_ref=src, dst_ref=dst, send_sem=ss, recv_sem=rs,
            device_id=dev, device_id_type=pl.DeviceIdType.MESH,
        )
        copy.start()
        pending.append(copy)
        return copy

    def await_all(copies):
        for copy in copies:
            copy.wait_recv()

    def landed(copies):
        stage("wait", await_all, copies)

    barrier = pltpu.get_barrier_semaphore()
    for d in range(1, n):
        pl.semaphore_signal(barrier, inc=1, device_id=to_lat(d), device_id_type=pl.DeviceIdType.MESH)
    for d in range(1, m):
        pl.semaphore_signal(barrier, inc=1, device_id=to_lon(d), device_id_type=pl.DeviceIdType.MESH)

    loads = []
    for k, (src, dst) in enumerate((
        (chan_h, chan_ref), (prec_h, prec_ref), (pred_h, pred_ref),
        (innov_h, innov_ref), (cell_h, cell_ref), (jac_h, jac_ref),
    )):
        copy = pltpu.make_async_copy(src, dst, in_s.at[k])
        copy.start()
        loads.append(copy)
    load_chan, load_prec, load_pred, load_innov, load_cell, load_jac = loads

    count = count_ref[0, 0]
    sub = lax.broadcasted_iota(jnp.int32, TILE, 0)
    slot8 = sub * OBS_BLOCK + lax.broadcasted_iota(jnp.int32, TILE, 1)

    def pairs_of(tile):
        return [
            jnp.concatenate([tile[2 * p : 2 * p + 1], tile[2 * p + 1 : 2 * p + 2]], axis=1)
            for p in range(PAIRS)
        ]

    def rows_of(row, count):
        packed = jnp.broadcast_to(row, (16, row.shape[1])).astype(BF16)
        return jnp.concatenate([packed] * (count // 16), axis=0)

    def stack_left(term, mask):
        high = term.astype(BF16).astype(F32)
        low = term - high
        sides = []
        for side in (high, low):
            twice = jnp.concatenate([side, side], axis=0).astype(BF16)
            sides.append(jnp.concatenate([twice] * (blocks // 2), axis=0) * mask)
        return jnp.concatenate(sides, axis=0)

    def add_table(lefts, hots):
        acc_ref[...] += lax.dot_general(
            jnp.concatenate(lefts, axis=1), jnp.concatenate(hots, axis=1), NT,
            preferred_element_type=F32,
        )

    def preds_of(it, p):
        start = pl.multiple_of((it * PAIRS + p) * PAIR, PAIR)
        return pred_ref[:, pl.ds(start, PAIR)]

    def write_table(s):
        half = NPRED * blocks
        for j in range(n * chunk):
            if j < width:
                top = (j // per) * NPRED
                lanes = slice((j % per) * LANES, (j % per + 1) * LANES)
                tile = acc_ref[top : top + NPRED, lanes] + acc_ref[half + top : half + top + NPRED, lanes]
            else:
                tile = jnp.zeros((NPRED, LANES), F32)
            table_ref[s, j // chunk, j % chunk] = tile

    def scatter(s):
        return [
            send(table_ref.at[s, lax.rem(me + d, n)], ta.at[s, d], ta_s.at[s, d], ta_r.at[s, d], to_lat(d))
            for d in range(1, n)
        ]

    def across(s, copies):
        landed(copies)
        bb[s, z] = total_of([table_ref[s, me]] + [ta[s, d] for d in range(1, n)])
        return [
            send(bb.at[s, z], bb.at[s, z], b_s.at[s, d], b_r.at[s, d], to_lon(d)) for d in range(1, m)
        ]

    def chunk_sum(s, copies):
        landed(copies)
        return total_of([bb[s, j] for j in range(m)])

    def gather(i, value):
        tf[i, me] = value
        return [
            send(tf.at[i, me], tf.at[i, me], c_s.at[i, d], c_r.at[i, d], to_lat(d)) for d in range(1, n)
        ]

    def lon_tile(e, tile):
        sz[e, z] = tile
        return [send(sz.at[e, z], sz.at[e, z], z_s.at[e, d], z_r.at[e, d], to_lon(d)) for d in range(1, m)]

    def lon_total(e, copies):
        landed(copies)
        return total_of([sz[e, j] for j in range(m)])

    def lat_tile(e, tile):
        sw[e, me] = tile
        return [send(sw.at[e, me], sw.at[e, me], w_s.at[e, d], w_r.at[e, d], to_lat(d)) for d in range(1, n)]

    def lat_total(e, copies):
        landed(copies)
        return jnp.sum(total_of([sw[e, j] for j in range(n)]), axis=1, keepdims=True)

    def rows_tile(*tiles):
        out = jnp.zeros(TILE, F32)
        for k, tile in enumerate(tiles):
            out = jnp.where(sub == k, jnp.sum(tile, axis=0, keepdims=True), out)
        return out

    def halo(k, field, cols):
        return [
            send(field.at[LAT_DEV - 1], hu.at[k], h_s.at[k, 0], h_r.at[k, 0], to_lat(1)),
            send(field.at[0], hd.at[k], h_s.at[k, 1], h_r.at[k, 1], to_lat(n - 1)),
            send(cols.at[1], hc.at[k, 0], h_s.at[k, 2], h_r.at[k, 2], to_lon(1)),
            send(cols.at[0], hc.at[k, 1], h_s.at[k, 3], h_r.at[k, 3], to_lon(m - 1)),
        ]

    load_chan.wait()
    load_prec.wait()
    load_pred.wait()
    stage("load", load_innov.wait)
    acc_ref[...] = jnp.zeros_like(acc_ref)
    iota_ch = lax.broadcasted_iota(jnp.int32, (CH_BLOCK, PAIR), 0).astype(F32).astype(BF16)
    iota_b = (lax.broadcasted_iota(jnp.int32, (NPRED * blocks, PAIR), 0) // NPRED).astype(F32).astype(BF16)
    one, none = jnp.ones((), BF16), jnp.zeros((), BF16)

    def square_step(step, carry):
        lefts, hots = [], []
        for g in range(SQUARE_STEP):
            it = step * SQUARE_STEP + g
            base = pl.multiple_of(it * LINES, LINES)
            w8 = jnp.where(base * OBS_BLOCK + slot8 < count, prec_ref[pl.ds(base, LINES), :], 0.0)
            w_ref[pl.ds(base, LINES), :] = w8
            y_ref[pl.ds(base, LINES), :] = w8 * innov_ref[pl.ds(base, LINES), :]
            weights = pairs_of(w8)
            chan8 = chan_ref[pl.ds(base, LINES), :]
            lows = pairs_of((chan8 % CH_BLOCK).astype(F32))
            tops = pairs_of((chan8 // CH_BLOCK).astype(F32))
            for p in range(PAIRS):
                hot = jnp.where(iota_ch == rows_of(lows[p], CH_BLOCK), one, none)
                mask = jnp.where(iota_b == rows_of(tops[p], NPRED * blocks), one, none)
                hot_ref[it * PAIRS + p] = hot
                msk_ref[it * PAIRS + p] = mask
                preds = preds_of(it, p)
                lefts.append(stack_left(preds * preds * weights[p], mask))
                hots.append(hot)
        add_table(lefts, hots)
        return carry

    stage("squares", lax.fori_loop, 0, groups // SQUARE_STEP, square_step, 0)
    stage("write", write_table, 0)

    load_cell.wait()
    first = jnp.broadcast_to(cell_ref[:, 0:1], (lines, LANES)) // LON_DEV
    iota_l = lax.broadcasted_iota(jnp.int32, (lines, LANES), 0)
    iota_r = lax.broadcasted_iota(jnp.int32, (lines, LANES), 1)
    turned = jnp.transpose(first)
    before = jnp.where((first == turned) & (iota_l < iota_r), iota_l, -1)
    before = jnp.max(before, axis=0, keepdims=True)
    last = jnp.max(jnp.where(first == iota_r, iota_l, -1), axis=0, keepdims=True)
    index_v[0:1, :] = turned[0:1, :]
    index_v[1:2, :] = jnp.where(before < 0, lines, before)
    index_v[2:3, :] = jnp.where(last < 0, lines, last)
    load_index = pltpu.make_async_copy(index_v, index_s, ix_s.at[0])
    load_index.start()

    stage("barrier", pl.semaphore_wait, barrier, n - 1 + m - 1)
    for j in range(own):
        own_all[z, j] = bprec_ref[:, j * LANES : (j + 1) * LANES]
    squares = scatter(0)
    owners = [send(own_all.at[z], own_all.at[z], o_s.at[d], o_r.at[d], to_lon(d)) for d in range(1, m)]

    def adjoint_bias(s):
        acc_ref[...] = jnp.zeros_like(acc_ref)

        def table_step(step, carry):
            lefts, hots = [], []
            for g in range(TABLE_STEP):
                it = step * TABLE_STEP + g
                values = pairs_of(y_ref[pl.ds(pl.multiple_of(it * LINES, LINES), LINES), :])
                for p in range(PAIRS):
                    lefts.append(stack_left(preds_of(it, p) * values[p], msk_ref[it * PAIRS + p]))
                    hots.append(hot_ref[it * PAIRS + p])
            add_table(lefts, hots)
            return carry

        stage("table", lax.fori_loop, 0, groups // TABLE_STEP, table_step, 0)
        stage("write", write_table, s)
        return scatter(s)

    iota_col = lax.broadcasted_iota(jnp.int32, (LON_DEV, OBS_BLOCK), 0)

    def jac_of(line):
        return jac_ref[pl.ds(pl.multiple_of(line * OBS_BLOCK, OBS_BLOCK), OBS_BLOCK), :]

    def adjoint_state(k):
        def line_step(step, carry):
            outs = []
            for g in range(ADJOINT_STEP):
                base = pl.multiple_of((step * ADJOINT_STEP + g) * LINES, LINES)
                cols = cell_ref[pl.ds(base, LINES), :] % LON_DEV
                values = y_ref[pl.ds(base, LINES), :]
                for l in range(0, LINES, 2):
                    rows = []
                    for j in (l, l + 1):
                        high, low = halves(jnp.where(iota_col == cols[j : j + 1, :], values[j : j + 1, :], 0.0))
                        rows.append(jnp.concatenate([high, low], axis=1))
                    jacs = jnp.concatenate([jac_of(base + l), jac_of(base + l + 1)], axis=1)
                    both = jnp.dot(
                        jnp.concatenate(rows, axis=0), jnp.concatenate([jacs, jacs], axis=0),
                        preferred_element_type=F32,
                    )
                    outs += [both[:LON_DEV, :LEV], both[LON_DEV:, LEV:]]
            first_line = step * ADJOINT_STEP * LINES
            for l in range(ADJOINT_STEP * LINES):
                part_ref[first_line + l] = outs[l] + part_ref[index_s[1, first_line + l]]
            return carry

        stage("adjoint", lax.fori_loop, 0, groups // ADJOINT_STEP, line_step, 0)

        def row_step(i, carry):
            row = part_ref[index_s[2, i]]
            g_ref[k, i] = row
            gc_ref[k, 0, pl.ds(i, 1), :] = row[0:1, :]
            gc_ref[k, 1, pl.ds(i, 1), :] = row[LON_DEV - 1 : LON_DEV, :]
            return carry

        stage("rows", lax.fori_loop, 0, LAT_DEV, row_step, 0)
        return halo(2 * k, g_ref.at[k], gc_ref.at[k])

    smooth = smooth_ref[0:1, :]
    top_keep = (me > 0).astype(F32)
    bottom_keep = (me < n - 1).astype(F32)
    column = lax.broadcasted_iota(jnp.int32, (LON_DEV, LEV), 0)
    zero = jnp.zeros((LON_DEV, LEV), F32)

    def sweep(field, k, use, acc):
        up, down, side = hu.at[k], hd.at[k], hc.at[k]

        def stencil(i, above, below):
            mid = field[i]
            left = jnp.where(column == 0, side[0, pl.ds(i, 1), :], pltpu.roll(mid, 1, 0))
            right = jnp.where(
                column == LON_DEV - 1, side[1, pl.ds(i, 1), :], pltpu.roll(mid, LON_DEV - 1, 0)
            )
            return mid + smooth * (above + below + left + right - 4.0 * mid)

        acc = use(0, stencil(0, up[...] * top_keep, field[1]), acc)
        inner = LAT_DEV - 2
        group = next(k for k in (5, 4, 3, 2, 1) if inner % k == 0)

        def rows(it, a):
            for k in range(group):
                i = 1 + it * group + k
                a = use(i, stencil(i, field[i - 1], field[i + 1]), a)
            return a

        acc = lax.fori_loop(0, inner // group, rows, acc)
        end = LAT_DEV - 1
        return use(end, stencil(end, field[end - 1], down[...] * bottom_keep), acc)

    def keep_columns(k, i, row):
        rc_ref[k, 0, pl.ds(i, 1), :] = row[0:1]
        rc_ref[k, 1, pl.ds(i, 1), :] = row[LON_DEV - 1 : LON_DEV]

    def forward_state(field, k, old):
        def use(i, row, acc):
            high, low = halves(row)
            split_ref[i] = jnp.concatenate([high, low], axis=1)
            return acc

        stage("sweep_u", sweep, field, k, use, 0)

        def line_step(step, carry):
            for g in range(FORWARD_STEP):
                base = pl.multiple_of((step * FORWARD_STEP + g) * LINES, LINES)
                cols = cell_ref[pl.ds(base, LINES), :] % LON_DEV
                seen = []
                for l in range(0, LINES, 2):
                    fields = [split_ref[index_s[0, base + j]] for j in (l, l + 1)]
                    jacs = jnp.concatenate([turned_ref[base + l], turned_ref[base + l + 1]], axis=1)
                    both = jnp.dot(
                        jnp.concatenate(fields, axis=0), jnp.concatenate([jacs, jacs], axis=0),
                        preferred_element_type=F32,
                    )
                    for j, part in ((l, both[:LON_DEV, :OBS_BLOCK]), (l + 1, both[LON_DEV:, OBS_BLOCK:])):
                        picked = jnp.where(iota_col == cols[j : j + 1, :], part, 0.0)
                        seen.append(jnp.sum(picked, axis=0, keepdims=True))
                y_ref[pl.ds(base, LINES), :] = jnp.concatenate(seen, axis=0)
            return carry

        stage("forward", lax.fori_loop, 0, groups // FORWARD_STEP, line_step, 0)

    def forward_bias(i, beta):
        for b in range(blocks):
            for h in range(per):
                j = b * per + h
                high, low = halves(tf[i, j // chunk, j % chunk])
                coef_ref[b * NPRED : (b + 1) * NPRED, h * LANES : (h + 1) * LANES] = high
                coef_ref[b * NPRED : (b + 1) * NPRED, CH_BLOCK + h * LANES : CH_BLOCK + (h + 1) * LANES] = low
        coef2 = coef_ref[...]

        def look_step(step, acc):
            for g in range(LOOK_STEP):
                it = step * LOOK_STEP + g
                base = pl.multiple_of(it * LINES, LINES)
                tops = pairs_of(chan_ref[pl.ds(base, LINES), :] // CH_BLOCK)
                looked = []
                for p in range(PAIRS):
                    hot = hot_ref[it * PAIRS + p]
                    mid = jnp.dot(coef2, jnp.concatenate([hot, hot], axis=0), preferred_element_type=F32)
                    which = jnp.broadcast_to(tops[p], (NPRED, PAIR))
                    total = jnp.zeros((NPRED, PAIR), F32)
                    for b in range(blocks):
                        total = jnp.where(which == b, mid[b * NPRED : (b + 1) * NPRED], total)
                    total = jnp.sum(total * preds_of(it, p), axis=0, keepdims=True)
                    looked += [total[:, :OBS_BLOCK], total[:, OBS_BLOCK:]]
                f8 = y_ref[pl.ds(base, LINES), :] + jnp.concatenate(looked, axis=0)
                if beta is not None:
                    f8 = f8 + beta * f_ref[pl.ds(base, LINES), :]
                y8 = w_ref[pl.ds(base, LINES), :] * f8
                f_ref[pl.ds(base, LINES), :] = f8
                y_ref[pl.ds(base, LINES), :] = y8
                acc = acc + y8 * f8
            return acc

        return stage("look", lax.fori_loop, 0, groups // LOOK_STEP, look_step, jnp.zeros(TILE, F32))

    def spread(column):
        return jnp.broadcast_to(column, TILE)

    def dots(*pairs):
        return [total_of([a[j] * b[j] for j in range(chunk)]) for a, b in pairs]

    part_ref[lines] = zero
    sums = adjoint_bias(1)
    squares = across(0, squares)
    stage("load_index", load_index.wait)
    stage("load_jac", load_jac.wait)
    halos = adjoint_state(0)
    sums = across(1, sums)

    def turn_step(it, carry):
        for l in range(LINES):
            turned_ref[it * LINES + l] = jnp.transpose(jac_of(it * LINES + l))
        return carry

    stage("turn", lax.fori_loop, 0, groups, turn_step, 0)
    landed(halos)

    def use_first(i, row, acc):
        r0_ref[i] = row
        keep_columns(0, i, row)
        return acc + row * row

    pp_state = fold(stage("sweep", sweep, g_ref.at[0], 0, use_first, zero))
    halos = halo(1, r0_ref, rc_ref.at[0])
    crossing = lon_tile(0, pp_state)
    landed(owners)
    for j in range(chunk):
        spot = jnp.minimum(me * chunk + j, width - 1)
        bp_c[j] = own_all[spot // own, lax.rem(spot, own)]
    diag_c[...] = bp_c[...] + chunk_sum(0, squares)
    r_c[...] = chunk_sum(1, sums)
    p_c[...] = r_c[...] / diag_c[...]
    gathers = gather(0, p_c[...])
    around = lat_tile(0, rows_tile(lon_total(0, crossing), *dots((r_c, p_c), (r_c, r_c))))
    landed(halos)
    forward_state(r0_ref, 1, None)
    landed(gathers)
    totals = lat_total(0, around)
    rz = spread(totals[0:1] + totals[1:2])
    norms = [spread(totals[0:1] + totals[2:3])]
    beta = None
    alphas = []
    for turn in range(ITERS):
        final = turn == ITERS - 1
        observed = forward_bias(turn, None if beta is None else beta[0:1])
        sums = adjoint_bias(2 + turn)
        if turn > 0:
            slope = beta[0:1]

            def p_step(it, acc):
                for k in range(4):
                    i = it * 4 + k
                    row = r1_ref[i] + slope * r0_ref[i]
                    p1_ref[i] = row
                    acc = acc + row * row
                return acc

            pp_state = fold(stage("p_step", lax.fori_loop, 0, LAT_DEV // 4, p_step, zero))
            p_c[...] = tf[turn, me] + beta * p_c[...]
        crossing = lon_tile(1 + 2 * turn, pp_state + observed)
        halos = adjoint_state(1 + turn)
        pp_bias = total_of([bp_c[j] * p_c[j] * p_c[j] for j in range(chunk)])
        around = lat_tile(1 + 2 * turn, rows_tile(lon_total(1 + 2 * turn, crossing), pp_bias))
        sums = across(2 + turn, sums)
        totals = lat_total(1 + 2 * turn, around)
        alpha = rz / spread(totals[0:1] + totals[1:2])
        alphas.append(alpha)
        line = alpha[0:1]
        landed(halos)
        p_ref, old_ref = (p1_ref, r1_ref) if turn > 0 else (r0_ref, r0_ref)

        def use_next(i, row, acc):
            new = old_ref[i] - line * (p_ref[i] + row)
            if not final:
                r1_ref[i] = new
                keep_columns(1, i, new)
            return acc + new * new

        rr_state = fold(stage("sweep", sweep, g_ref.at[1 + turn], 2 + 2 * turn, use_next, zero))
        crossing = lon_tile(2 + 2 * turn, rr_state)
        if not final:
            halos = halo(3 + 2 * turn, r1_ref, rc_ref.at[1])
        image = bp_c[...] * p_c[...] + chunk_sum(2 + turn, sums)
        r_c[...] = r_c[...] - alpha * image
        z_c = r_c[...] / diag_c[...]
        if not final:
            gathers = gather(turn + 1, z_c)
        around = lat_tile(
            2 + 2 * turn, rows_tile(lon_total(2 + 2 * turn, crossing), *dots((r_c, z_c), (r_c, r_c)))
        )
        if not final:
            landed(halos)
            forward_state(r1_ref, 3 + 2 * turn, None)
            landed(gathers)
        else:
            first_line, last_line = alphas[0][0:1], alphas[1][0:1]

            def x_step(it, carry):
                for k in range(4):
                    i = it * 4 + k
                    x_out[i] = first_line * r0_ref[i] + last_line * p1_ref[i]
                return carry

            stage("x_step", lax.fori_loop, 0, LAT_DEV // 4, x_step, 0)
            for j in range(own):
                spot = z * own + j
                row, col = spot // chunk, lax.rem(spot, chunk)
                start = tf[0, row, col]
                bias_out[:, j * LANES : (j + 1) * LANES] = alphas[0] * start + alphas[1] * (
                    tf[1, row, col] + beta * start
                )
        totals = lat_total(2 + 2 * turn, around)
        new = spread(totals[0:1] + totals[1:2])
        norms.append(spread(totals[0:1] + totals[2:3]))
        beta = new / rz
        rz = new
    lane = lax.broadcasted_iota(jnp.int32, TILE, 1)
    squares = jnp.zeros(TILE, F32)
    for j in range(ITERS + 1):
        squares = jnp.where(lane == j, norms[j], squares)
    norms_out[...] = jnp.sqrt(squares)
    for copy in pending:
        copy.wait_send()


def publish(x_ref, bias_ref, norms_ref, x_out, bias_out, norms_out, row_ref, sems):
    row_ref[...] = norms_ref[0, : row_ref.shape[0]]
    copies = [
        pltpu.make_async_copy(src, dst, sems.at[k])
        for k, (src, dst) in enumerate(((x_ref, x_out), (bias_ref, bias_out), (row_ref, norms_out)))
    ]
    for copy in copies:
        copy.start()
    for copy in copies:
        copy.wait()


def shaped(*shape):
    return jax.ShapeDtypeStruct(shape, F32)


def body(
    innovations,
    obs_precision,
    jacobian,
    predictors,
    obs_column,
    obs_channel,
    obs_count,
    smoothing,
    bias_precision,
):
    n = lax.axis_size("swath")
    m = lax.axis_size("chan")
    owned_width = bias_precision.shape[1]
    own = owned_width // LANES
    width = own * m
    blocks = owned_width * m // CH_BLOCK
    slots = obs_precision.shape[0]
    lines = slots // OBS_BLOCK
    chunk = -(-width // n)
    half = NPRED * blocks
    grid_lines = lambda a: a.reshape(lines, OBS_BLOCK)
    held = lambda a: pltpu.with_memory_space_constraint(a, pltpu.HBM)
    vm = lambda *s: pltpu.VMEM(s, F32)
    vb = lambda *s: pltpu.VMEM(s, BF16)
    vi = lambda *s: pltpu.VMEM(s, jnp.int32)
    sem = lambda *s: pltpu.SemaphoreType.DMA(s)
    halos = 1 + 2 * ITERS
    tables = 2 + ITERS
    events = 1 + 2 * ITERS
    scratch = [
        vi(lines, OBS_BLOCK), vi(lines, OBS_BLOCK), vm(lines, OBS_BLOCK), vm(lines, OBS_BLOCK),
        vm(NPRED, slots), vb(slots, LEV),
        vb(lines, LEV, OBS_BLOCK), vb(lines // 2, CH_BLOCK, PAIR), vb(lines // 2, half, PAIR),
        vm(lines, OBS_BLOCK), vm(lines, OBS_BLOCK), vm(lines, OBS_BLOCK), vm(lines + 1, LON_DEV, LEV),
        vi(8, LANES), pltpu.SMEM((8, LANES), jnp.int32),
        vm(1 + ITERS, LAT_DEV, LON_DEV, LEV), vm(1 + ITERS, 2, LAT_DEV, LEV),
        vm(LAT_DEV, LON_DEV, LEV), vm(LAT_DEV, LON_DEV, LEV), vm(LAT_DEV, LON_DEV, LEV),
        vm(2, 2, LAT_DEV, LEV), vb(LAT_DEV, LON_DEV, 2 * LEV),
        vm(2 * half, CH_BLOCK), vm(tables, n, chunk, NPRED, LANES), vb(half, 2 * CH_BLOCK),
        vm(chunk, NPRED, LANES), vm(chunk, NPRED, LANES), vm(chunk, NPRED, LANES),
        vm(chunk, NPRED, LANES), vm(m, own, NPRED, LANES),
        vm(halos, LON_DEV, LEV), vm(halos, LON_DEV, LEV), vm(halos, 2, LAT_DEV, LEV),
        vm(tables, n, chunk, NPRED, LANES), vm(tables, m, chunk, NPRED, LANES),
        vm(ITERS, n, chunk, NPRED, LANES), vm(events, m, 8, LANES), vm(events, n, 8, LANES),
        sem(6), sem(1), sem(m), sem(m), sem(halos, 4), sem(halos, 4), sem(tables, n), sem(tables, n),
        sem(tables, m), sem(tables, m), sem(ITERS, n), sem(ITERS, n), sem(events, m), sem(events, m),
        sem(events, n), sem(events, n),
    ]
    VM = pl.BlockSpec(memory_space=pltpu.VMEM)
    HB = pl.BlockSpec(memory_space=pltpu.HBM)
    x, bias, norms = pl.pallas_call(
        functools.partial(kernel, n, m, own, blocks, lines, chunk),
        out_shape=(shaped(LAT_DEV, LON_DEV, LEV), shaped(NPRED, owned_width), shaped(8, LANES)),
        in_specs=[pl.BlockSpec(memory_space=pltpu.SMEM), VM, VM] + [HB] * 6,
        out_specs=(VM, VM, VM),
        scratch_shapes=scratch,
        compiler_params=pltpu.CompilerParams(
            collective_id=0, has_side_effects=True, vmem_limit_bytes=VMEM_LIMIT
        ),
        name="cg",
    )(
        obs_count, held(smoothing.reshape(1, LEV)), held(bias_precision),
        held(grid_lines(obs_column)), held(grid_lines(obs_channel)), held(grid_lines(obs_precision)),
        held(grid_lines(innovations)), held(predictors), held(jacobian),
    )
    kept = (x.shape, bias.shape, (ITERS + 1,))
    return pl.pallas_call(
        publish,
        out_shape=tuple(shaped(*shape) for shape in kept),
        in_specs=[VM, VM, VM],
        out_specs=(HB, HB, HB),
        scratch_shapes=[vm(ITERS + 1), sem(3)],
        compiler_params=pltpu.CompilerParams(vmem_limit_bytes=4 * 1024 * 1024),
        name="publish",
    )(x, bias, norms)


def solution(mesh):
    placed = (
        P(("swath", "chan")),
        P(("swath", "chan")),
        P(("swath", "chan"), None),
        P(None, ("swath", "chan")),
        P(("swath", "chan")),
        P(("swath", "chan")),
        P("swath", "chan"),
        P(),
        P(None, "chan"),
    )
    return jax.shard_map(
        body,
        mesh=mesh,
        in_specs=placed,
        out_specs=(P("swath", "chan", None), P(None, "chan"), P()),
        check_vma=False,
    )
```

```python
import functools

import jax
import jax.numpy as jnp
from jax import lax
from jax.experimental import pallas as pl
from jax.experimental.pallas import tpu as pltpu
from jax.sharding import PartitionSpec as P

LEV = 128
NPRED = 8
CH_BLOCK = 256
OBS_BLOCK = 128
LAT_DEV = 32
LON_DEV = 64
ITERS = 2
LINES = 8
PAIRS = LINES // 2
SQUARE_STEP, TABLE_STEP, LOOK_STEP, ADJOINT_STEP, FORWARD_STEP = 4, 8, 8, 4, 4
PAIR = 2 * OBS_BLOCK
LANES = 128
PIECES = 2
TILE = (8, LANES)
F32 = jnp.float32
BF16 = jnp.bfloat16
NT = (((1,), (1,)), ((), ()))
VMEM_LIMIT = 44 * 1024 * 1024


def halves(value):
    high = value.astype(BF16)
    return high, (value - high.astype(F32)).astype(BF16)


def fold(value):
    total = value[0:8]
    for i in range(1, value.shape[0] // 8):
        total = total + value[8 * i : 8 * i + 8]
    return total


def total_of(parts):
    total = parts[0]
    for part in parts[1:]:
        total = total + part
    return total


def stage(name, run, *args):
    return run(*args)


def kernel(n, m, own, blocks, lines, chunk, *refs):
    refs = list(refs)
    take = lambda k: [refs.pop(0) for _ in range(k)]
    count_ref, smooth_ref, bprec_ref = take(3)
    cell_h, chan_h, prec_h, innov_h, pred_h, jac_h = take(6)
    x_out, bias_out, norms_out = take(3)
    cell_ref, chan_ref, prec_ref, innov_ref, pred_ref, jac_ref = take(6)
    turned_ref, hot_ref, msk_ref, w_ref, y_ref, f_ref, part_ref = take(7)
    index_v, index_s = take(2)
    g_ref, gc_ref, r0_ref, r1_ref, p1_ref, q_ref, s_ref, kept_ref, split_ref = take(9)
    acc_ref, table_ref, coef_ref = take(3)
    bp_c, diag_c, r_c, p_c, z_c, q_c, own_ref = take(7)
    hv, hc, hx, rim_rows, rim_cols, ta, bb, tf, sz, sw = take(10)
    in_s, ix_s, o_s, o_r, h_s, h_r, ta_s, ta_r, b_s, b_r, c_s, c_r, z_s, z_r, w_s, w_r = take(16)
    width = own * m
    groups = lines // LINES
    me = lax.axis_index("swath")
    z = lax.axis_index("chan")
    per = CH_BLOCK // LANES
    count = min(PIECES, chunk)
    cuts = [chunk * k // count for k in range(count + 1)]
    pieces = [pl.ds(a, b - a) for a, b in zip(cuts, cuts[1:])]

    def to_lat(d):
        return {"swath": lax.rem(me + d, n)}

    def to_lon(d):
        return {"chan": lax.rem(z + d, m)}

    pending = []

    def send(src, dst, ss, rs, dev):
        copy = pltpu.make_async_remote_copy(
            src_ref=src, dst_ref=dst, send_sem=ss, recv_sem=rs,
            device_id=dev, device_id_type=pl.DeviceIdType.MESH,
        )
        copy.start()

    def sent(ref, ss, rs):
        group = pltpu.make_async_remote_copy(
            src_ref=ref, dst_ref=ref, send_sem=ss, recv_sem=rs,
            device_id=to_lon(1), device_id_type=pl.DeviceIdType.MESH,
        )
        pending.append(group)
        return group

    def await_all(copies):
        for copy in copies:
            copy.wait_recv()

    def landed(copies):
        stage("wait", await_all, copies)

    def diagonal(d, e):
        return {"swath": lax.rem(me + d, n), "chan": lax.rem(z + e, m)}

    corners = [(1, 1), (1, m - 1), (n - 1, 1), (n - 1, m - 1)]
    barrier = pltpu.get_barrier_semaphore()
    for d in range(1, n):
        pl.semaphore_signal(barrier, inc=1, device_id=to_lat(d), device_id_type=pl.DeviceIdType.MESH)
    for d in range(1, m):
        pl.semaphore_signal(barrier, inc=1, device_id=to_lon(d), device_id_type=pl.DeviceIdType.MESH)

    for d, e in corners:
        pl.semaphore_signal(
            barrier, inc=1, device_id=diagonal(d, e), device_id_type=pl.DeviceIdType.MESH
        )

    loads = []
    for k, (src, dst) in enumerate((
        (chan_h, chan_ref), (prec_h, prec_ref), (pred_h, pred_ref),
        (innov_h, innov_ref), (cell_h, cell_ref), (jac_h, jac_ref),
    )):
        copy = pltpu.make_async_copy(src, dst, in_s.at[k])
        copy.start()
        loads.append(copy)
    load_chan, load_prec, load_pred, load_innov, load_cell, load_jac = loads

    count = count_ref[0, 0]
    sub = lax.broadcasted_iota(jnp.int32, TILE, 0)
    slot8 = sub * OBS_BLOCK + lax.broadcasted_iota(jnp.int32, TILE, 1)

    def pairs_of(tile):
        return [
            jnp.concatenate([tile[2 * p : 2 * p + 1], tile[2 * p + 1 : 2 * p + 2]], axis=1)
            for p in range(PAIRS)
        ]

    def rows_of(row, count):
        packed = jnp.broadcast_to(row, (16, row.shape[1])).astype(BF16)
        return jnp.concatenate([packed] * (count // 16), axis=0)

    def stack_left(term, mask):
        high = term.astype(BF16).astype(F32)
        low = term - high
        sides = []
        for side in (high, low):
            twice = jnp.concatenate([side, side], axis=0).astype(BF16)
            sides.append(jnp.concatenate([twice] * (blocks // 2), axis=0) * mask)
        return jnp.concatenate(sides, axis=0)

    def add_table(lefts, hots):
        acc_ref[...] += lax.dot_general(
            jnp.concatenate(lefts, axis=1), jnp.concatenate(hots, axis=1), NT,
            preferred_element_type=F32,
        )

    def preds_of(it, p):
        start = pl.multiple_of((it * PAIRS + p) * PAIR, PAIR)
        return pred_ref[:, pl.ds(start, PAIR)]

    def write_table(s):
        half = NPRED * blocks
        for j in range(n * chunk):
            if j < width:
                top = (j // per) * NPRED
                lanes = slice((j % per) * LANES, (j % per + 1) * LANES)
                tile = acc_ref[top : top + NPRED, lanes] + acc_ref[half + top : half + top + NPRED, lanes]
            else:
                tile = jnp.zeros((NPRED, LANES), F32)
            table_ref[s, j // chunk, j % chunk] = tile

    def scatter(s):
        groups = []
        for k, part in enumerate(pieces):
            for d in range(1, n):
                send(
                    table_ref.at[s, lax.rem(me + d, n), part], ta.at[s, d, part],
                    ta_s.at[s, k], ta_r.at[s, k], to_lat(d),
                )
            groups.append(sent(ta.at[s, pl.ds(1, n - 1), part], ta_s.at[s, k], ta_r.at[s, k]))
        return groups

    def across(s, arriving, between=None):
        leaving = []
        for k, part in enumerate(pieces):
            if between is not None:
                between(k)
            landed([arriving[k]])
            bb[s, z, part] = total_of([table_ref[s, me, part]] + [ta[s, d, part] for d in range(1, n)])
            for d in range(1, m):
                send(bb.at[s, z, part], bb.at[s, z, part], b_s.at[s, k], b_r.at[s, k], to_lon(d))
            leaving.append(sent(bb.at[s, pl.ds(0, m - 1), part], b_s.at[s, k], b_r.at[s, k]))
        return leaving

    def chunk_sum(s, k, arriving):
        landed([arriving[k]])
        return total_of([bb[s, j, pieces[k]] for j in range(m)])

    def gather(i, k, value):
        part = pieces[k]
        tf[i, me, part] = value
        for d in range(1, n):
            send(tf.at[i, me, part], tf.at[i, me, part], c_s.at[i, k], c_r.at[i, k], to_lat(d))
        return [sent(tf.at[i, pl.ds(0, n - 1), part], c_s.at[i, k], c_r.at[i, k])]

    def lon_tile(e, tile):
        sz[e, z] = tile
        for d in range(1, m):
            send(sz.at[e, z], sz.at[e, z], z_s.at[e], z_r.at[e], to_lon(d))
        return [sent(sz.at[e, pl.ds(0, m - 1)], z_s.at[e], z_r.at[e])]

    def lon_total(e, copies):
        landed(copies)
        return total_of([sz[e, j] for j in range(m)])

    def lat_tile(e, tile):
        sw[e, me] = tile
        for d in range(1, n):
            send(sw.at[e, me], sw.at[e, me], w_s.at[e], w_r.at[e], to_lat(d))
        return [sent(sw.at[e, pl.ds(0, n - 1)], w_s.at[e], w_r.at[e])]

    def lat_total(e, copies):
        landed(copies)
        return jnp.sum(total_of([sw[e, j] for j in range(n)]), axis=1, keepdims=True)

    def rows_tile(*tiles):
        out = jnp.zeros(TILE, F32)
        for k, tile in enumerate(tiles):
            out = jnp.where(sub == k, jnp.sum(tile, axis=0, keepdims=True), out)
        return out

    def halo(k, wide):
        field, cols = g_ref.at[k], gc_ref.at[k]
        count = 2 if wide else 1
        last = pl.ds(LAT_DEV - count, count)
        near = pl.ds(0, count)
        far = pl.ds(2 - count, count)
        moves = [
            (0, field.at[last], hv.at[k, 0, far], to_lat(1)),
            (0, field.at[near], hv.at[k, 1, near], to_lat(n - 1)),
            (1, cols.at[1, far], hc.at[k, 0, far], to_lon(1)),
            (1, cols.at[0, near], hc.at[k, 1, near], to_lon(m - 1)),
        ]
        groups = [hv.at[k, pl.ds(0, 2), near], hc.at[k, pl.ds(0, 2), near]]
        if wide:
            top, end = pl.ds(0, 1), pl.ds(LAT_DEV - 1, 1)
            sources = (cols.at[1, 1, end], cols.at[0, 0, end], cols.at[1, 1, top], cols.at[0, 0, top])
            for q, (src, (d, e)) in enumerate(zip(sources, corners)):
                moves.append((2, src, hx.at[k, q, top], diagonal(d, e)))
            groups.append(hx.at[k, pl.ds(0, len(corners)), top])
        for j, src, dst, dev in moves:
            send(src, dst, h_s.at[k, j], h_r.at[k, j], dev)
        return [sent(ref, h_s.at[k, j], h_r.at[k, j]) for j, ref in enumerate(groups)]

    load_chan.wait()
    load_prec.wait()
    load_pred.wait()
    stage("load", load_innov.wait)
    acc_ref[...] = jnp.zeros_like(acc_ref)
    iota_ch = lax.broadcasted_iota(jnp.int32, (CH_BLOCK, PAIR), 0).astype(F32).astype(BF16)
    iota_b = (lax.broadcasted_iota(jnp.int32, (NPRED * blocks, PAIR), 0) // NPRED).astype(F32).astype(BF16)
    one, none = jnp.ones((), BF16), jnp.zeros((), BF16)

    def square_step(step, carry):
        lefts, hots = [], []
        for g in range(SQUARE_STEP):
            it = step * SQUARE_STEP + g
            base = pl.multiple_of(it * LINES, LINES)
            w8 = jnp.where(base * OBS_BLOCK + slot8 < count, prec_ref[pl.ds(base, LINES), :], 0.0)
            w_ref[pl.ds(base, LINES), :] = w8
            y_ref[pl.ds(base, LINES), :] = w8 * innov_ref[pl.ds(base, LINES), :]
            weights = pairs_of(w8)
            chan8 = chan_ref[pl.ds(base, LINES), :]
            lows = pairs_of((chan8 % CH_BLOCK).astype(F32))
            tops = pairs_of((chan8 // CH_BLOCK).astype(F32))
            for p in range(PAIRS):
                hot = jnp.where(iota_ch == rows_of(lows[p], CH_BLOCK), one, none)
                mask = jnp.where(iota_b == rows_of(tops[p], NPRED * blocks), one, none)
                hot_ref[it * PAIRS + p] = hot
                msk_ref[it * PAIRS + p] = mask
                preds = preds_of(it, p)
                lefts.append(stack_left(preds * preds * weights[p], mask))
                hots.append(hot)
        add_table(lefts, hots)
        return carry

    stage("squares", lax.fori_loop, 0, groups // SQUARE_STEP, square_step, 0)
    stage("write", write_table, 0)

    load_cell.wait()
    first = jnp.broadcast_to(cell_ref[:, 0:1], (lines, LANES)) // LON_DEV
    iota_l = lax.broadcasted_iota(jnp.int32, (lines, LANES), 0)
    iota_r = lax.broadcasted_iota(jnp.int32, (lines, LANES), 1)
    turned = jnp.transpose(first)
    before = jnp.where((first == turned) & (iota_l < iota_r), iota_l, -1)
    before = jnp.max(before, axis=0, keepdims=True)
    last = jnp.max(jnp.where(first == iota_r, iota_l, -1), axis=0, keepdims=True)
    index_v[0:1, :] = turned[0:1, :]
    index_v[1:2, :] = jnp.where(before < 0, lines, before)
    index_v[2:3, :] = jnp.where(last < 0, lines, last)
    load_index = pltpu.make_async_copy(index_v, index_s, ix_s.at[0])
    load_index.start()

    stage("barrier", pl.semaphore_wait, barrier, n - 1 + m - 1 + len(corners))
    squares = scatter(0)
    spots = [jnp.minimum(me * chunk + j, width - 1) for j in range(chunk)]
    for j in range(own):
        own_ref[j] = bprec_ref[:, j * LANES : (j + 1) * LANES]

    def bias_copy(j, d):
        return pltpu.make_async_remote_copy(
            src_ref=own_ref.at[lax.rem(spots[j], own)], dst_ref=bp_c.at[j], send_sem=o_s.at[j],
            recv_sem=o_r.at[j], device_id=to_lon(d), device_id_type=pl.DeviceIdType.MESH,
        )

    for j in range(chunk):
        @pl.when(spots[j] // own == z)
        def _():
            for d in range(1, m):
                bias_copy(j, d).start()
            bp_c[j] = own_ref[lax.rem(spots[j], own)]

    def adjoint_bias(s):
        acc_ref[...] = jnp.zeros_like(acc_ref)

        def table_step(step, carry):
            lefts, hots = [], []
            for g in range(TABLE_STEP):
                it = step * TABLE_STEP + g
                values = pairs_of(y_ref[pl.ds(pl.multiple_of(it * LINES, LINES), LINES), :])
                for p in range(PAIRS):
                    lefts.append(stack_left(preds_of(it, p) * values[p], msk_ref[it * PAIRS + p]))
                    hots.append(hot_ref[it * PAIRS + p])
            add_table(lefts, hots)
            return carry

        stage("table", lax.fori_loop, 0, groups // TABLE_STEP, table_step, 0)
        stage("write", write_table, s)
        return scatter(s)

    iota_col = lax.broadcasted_iota(jnp.int32, (LON_DEV, OBS_BLOCK), 0)

    def jac_of(line):
        return jac_ref[pl.ds(pl.multiple_of(line * OBS_BLOCK, OBS_BLOCK), OBS_BLOCK), :]

    def adjoint_state(k):
        def line_step(step, carry):
            outs = []
            for g in range(ADJOINT_STEP):
                base = pl.multiple_of((step * ADJOINT_STEP + g) * LINES, LINES)
                cols = cell_ref[pl.ds(base, LINES), :] % LON_DEV
                values = y_ref[pl.ds(base, LINES), :]
                for l in range(0, LINES, 2):
                    rows = []
                    for j in (l, l + 1):
                        high, low = halves(jnp.where(iota_col == cols[j : j + 1, :], values[j : j + 1, :], 0.0))
                        rows.append(jnp.concatenate([high, low], axis=1))
                    jacs = jnp.concatenate([jac_of(base + l), jac_of(base + l + 1)], axis=1)
                    both = jnp.dot(
                        jnp.concatenate(rows, axis=0), jnp.concatenate([jacs, jacs], axis=0),
                        preferred_element_type=F32,
                    )
                    outs += [both[:LON_DEV, :LEV], both[LON_DEV:, LEV:]]
            first_line = step * ADJOINT_STEP * LINES
            for l in range(ADJOINT_STEP * LINES):
                part_ref[first_line + l] = outs[l] + part_ref[index_s[1, first_line + l]]
            return carry

        stage("adjoint", lax.fori_loop, 0, groups // ADJOINT_STEP, line_step, 0)

        def row_step(i, carry):
            row = part_ref[index_s[2, i]]
            g_ref[k, i] = row
            for c in range(2):
                gc_ref[k, 0, c, pl.ds(i, 1), :] = row[c : c + 1, :]
                gc_ref[k, 1, c, pl.ds(i, 1), :] = row[LON_DEV - 2 + c : LON_DEV - 1 + c, :]
            return carry

        stage("rows", lax.fori_loop, 0, LAT_DEV, row_step, 0)
        return halo(k, k < ITERS)

    smooth = smooth_ref[0:1, :]
    top_keep = (me > 0).astype(F32)
    bottom_keep = (me < n - 1).astype(F32)
    column = lax.broadcasted_iota(jnp.int32, (LON_DEV, LEV), 0)
    zero = jnp.zeros((LON_DEV, LEV), F32)

    def relaxed(mid, above, below, left, right):
        return mid + smooth * (above + below + left + right - 4.0 * mid)

    def rim(k):
        field, cols, side = g_ref.at[k], gc_ref.at[k], hc.at[k]
        south_west, south_east, north_west, north_east = [hx[k, q, 0:1, :] for q in range(4)]
        lats = lax.broadcasted_iota(jnp.int32, (LAT_DEV, LEV), 0)

        def row(mid, above, below, west, east, keep):
            left = jnp.where(column == 0, west, pltpu.roll(mid, 1, 0))
            right = jnp.where(column == LON_DEV - 1, east, pltpu.roll(mid, LON_DEV - 1, 0))
            return relaxed(mid, above, below, left, right) * keep

        def col(mid, left, right, north, south):
            above = jnp.where(lats == 0, north * top_keep, pltpu.roll(mid, 1, 0))
            below = jnp.where(lats == LAT_DEV - 1, south * bottom_keep, pltpu.roll(mid, LAT_DEV - 1, 0))
            return relaxed(mid, above, below, left, right)

        rim_rows[0] = row(hv[k, 0, 1], hv[k, 0, 0], field[0], south_west, south_east, top_keep)
        rim_rows[1] = row(hv[k, 1, 0], field[LAT_DEV - 1], hv[k, 1, 1], north_west, north_east, bottom_keep)
        rim_cols[0] = col(side[0, 1], side[0, 0], cols[0, 0], south_west, north_west)
        rim_cols[1] = col(side[1, 0], cols[1, 1], side[1, 1], south_east, north_east)

    def sweep(field, up, down, west, east, use, acc):
        def stencil(i, above, below):
            mid = field[i]
            left = jnp.where(column == 0, west[pl.ds(i, 1), :], pltpu.roll(mid, 1, 0))
            right = jnp.where(
                column == LON_DEV - 1, east[pl.ds(i, 1), :], pltpu.roll(mid, LON_DEV - 1, 0)
            )
            return relaxed(mid, above, below, left, right)

        acc = use(0, stencil(0, up, field[1]), acc)
        inner = LAT_DEV - 2
        group = next(k for k in (5, 4, 3, 2, 1) if inner % k == 0)

        def rows(it, a):
            for k in range(group):
                i = 1 + it * group + k
                a = use(i, stencil(i, field[i - 1], field[i + 1]), a)
            return a

        acc = lax.fori_loop(0, inner // group, rows, acc)
        end = LAT_DEV - 1
        return use(end, stencil(end, field[end - 1], down), acc)

    def first_sweep(k, use):
        return fold(stage(
            "sweep", sweep, g_ref.at[k], hv[k, 0, 1] * top_keep, hv[k, 1, 0] * bottom_keep,
            hc.at[k, 0, 1], hc.at[k, 1, 0], use, zero,
        ))

    def second_sweep(k, field):
        def use(i, row, acc):
            high, low = halves(row)
            split_ref[i] = jnp.concatenate([high, low], axis=1)
            return acc

        rim(k)
        stage(
            "sweep_u", sweep, field, rim_rows[0], rim_rows[1], rim_cols.at[0], rim_cols.at[1], use, 0
        )

    def observe_state():
        def line_step(step, carry):
            for g in range(FORWARD_STEP):
                base = pl.multiple_of((step * FORWARD_STEP + g) * LINES, LINES)
                cols = cell_ref[pl.ds(base, LINES), :] % LON_DEV
                seen = []
                for l in range(0, LINES, 2):
                    fields = [split_ref[index_s[0, base + j]] for j in (l, l + 1)]
                    jacs = jnp.concatenate([turned_ref[base + l], turned_ref[base + l + 1]], axis=1)
                    both = jnp.dot(
                        jnp.concatenate(fields, axis=0), jnp.concatenate([jacs, jacs], axis=0),
                        preferred_element_type=F32,
                    )
                    for j, part in ((l, both[:LON_DEV, :OBS_BLOCK]), (l + 1, both[LON_DEV:, OBS_BLOCK:])):
                        picked = jnp.where(iota_col == cols[j : j + 1, :], part, 0.0)
                        seen.append(jnp.sum(picked, axis=0, keepdims=True))
                y_ref[pl.ds(base, LINES), :] = jnp.concatenate(seen, axis=0)
            return carry

        stage("forward", lax.fori_loop, 0, groups // FORWARD_STEP, line_step, 0)

    def forward_bias(i):
        for b in range(blocks):
            for h in range(per):
                j = b * per + h
                high, low = halves(tf[i, j // chunk, j % chunk])
                coef_ref[b * NPRED : (b + 1) * NPRED, h * LANES : (h + 1) * LANES] = high
                coef_ref[b * NPRED : (b + 1) * NPRED, CH_BLOCK + h * LANES : CH_BLOCK + (h + 1) * LANES] = low
        coef2 = coef_ref[...]

        def look_step(step, acc):
            for g in range(LOOK_STEP):
                it = step * LOOK_STEP + g
                base = pl.multiple_of(it * LINES, LINES)
                tops = pairs_of(chan_ref[pl.ds(base, LINES), :] // CH_BLOCK)
                looked = []
                for p in range(PAIRS):
                    hot = hot_ref[it * PAIRS + p]
                    mid = jnp.dot(coef2, jnp.concatenate([hot, hot], axis=0), preferred_element_type=F32)
                    which = jnp.broadcast_to(tops[p], (NPRED, PAIR))
                    total = jnp.zeros((NPRED, PAIR), F32)
                    for b in range(blocks):
                        total = jnp.where(which == b, mid[b * NPRED : (b + 1) * NPRED], total)
                    total = jnp.sum(total * preds_of(it, p), axis=0, keepdims=True)
                    looked += [total[:, :OBS_BLOCK], total[:, OBS_BLOCK:]]
                f8 = kept_ref[i, pl.ds(base, LINES), :] + jnp.concatenate(looked, axis=0)
                y8 = w_ref[pl.ds(base, LINES), :] * f8
                f_ref[i, pl.ds(base, LINES), :] = f8
                y_ref[pl.ds(base, LINES), :] = y8
                acc = acc + y8 * f8
            return acc

        return stage("look", lax.fori_loop, 0, groups // LOOK_STEP, look_step, jnp.zeros(TILE, F32))

    def spread(column):
        return jnp.broadcast_to(column, TILE)

    def dots(*pairs):
        return [total_of([a[j] * b[j] for j in range(chunk)]) for a, b in pairs]

    part_ref[lines] = zero
    sums = adjoint_bias(1)
    load_index.wait()
    stage("load_jac", load_jac.wait)
    halos = adjoint_state(0)
    squares = across(0, squares)

    def turn_step(it, carry):
        for l in range(LINES):
            turned_ref[it * LINES + l] = jnp.transpose(jac_of(it * LINES + l))
        return carry

    turns = [groups * k // len(pieces) for k in range(len(pieces) + 1)]

    def turn_some(k):
        stage("turn", lax.fori_loop, turns[k], turns[k + 1], turn_step, 0)

    sums = across(1, sums, turn_some)
    landed(halos)

    def use_first(i, row, acc):
        r0_ref[i] = row
        return acc + row * row

    pp_state = first_sweep(0, use_first)
    crossing = lon_tile(0, pp_state)
    second_sweep(0, r0_ref)
    for j in range(chunk):
        @pl.when(spots[j] // own != z)
        def _():
            bias_copy(j, 1).wait_recv()

    gathers = []
    for k, part in enumerate(pieces):
        diag_c[part] = bp_c[part] + chunk_sum(0, k, squares)
        r_c[part] = chunk_sum(1, k, sums)
        z_c[part] = r_c[part] / diag_c[part]
        p_c[part] = z_c[part]
        gathers += gather(0, k, z_c[part])
    observe_state()
    kept_ref[0] = y_ref[...]
    opening = lat_tile(0, rows_tile(lon_total(0, crossing), *dots((r_c, p_c), (r_c, r_c))))
    landed(gathers)
    alphas, norms = [], []
    beta = None
    for turn in range(ITERS):
        first, final = turn == 0, turn == ITERS - 1
        event = 1 + 2 * turn
        observed = forward_bias(turn)
        totals = lat_total(event - 1, opening)
        new = spread(totals[0:1] + totals[1:2])
        norms.append(spread(totals[0:1] + totals[2:3]))
        if not first:
            beta = new / rz
            slope = beta[0:1]

            def p_step(it, acc):
                for k in range(4):
                    i = it * 4 + k
                    row = r1_ref[i] + slope * r0_ref[i]
                    p1_ref[i] = row
                    acc = acc + row * row
                return acc

            pp_state = fold(stage("p_step", lax.fori_loop, 0, LAT_DEV // 4, p_step, zero))
            joined = f_ref[turn] + slope * f_ref[turn - 1]
            observed = fold(w_ref[...] * joined * joined)
            p_c[...] = z_c[...] + beta * p_c[...]
        rz = new
        crossing = lon_tile(event, pp_state + observed)
        sums = adjoint_bias(2 + turn)
        pp_bias = total_of([bp_c[j] * p_c[j] * p_c[j] for j in range(chunk)])
        around = lat_tile(event, rows_tile(lon_total(event, crossing), pp_bias))
        halos = adjoint_state(1 + turn)
        sums = across(2 + turn, sums)
        totals = lat_total(event, around)
        alpha = rz / spread(totals[0:1] + totals[1:2])
        alphas.append(alpha)
        line = alpha[0:1]
        landed(halos)
        old_ref = r0_ref if first else r1_ref

        def use_next(i, row, acc):
            image = old_ref[i] + row
            if first:
                q_ref[i] = image
                s_ref[i] = row
            else:
                image = image + slope * q_ref[i]
            residual = old_ref[i] - line * image
            if not final:
                r1_ref[i] = residual
            return acc + residual * residual

        crossing = lon_tile(event + 1, first_sweep(1 + turn, use_next))
        gathers = []
        for k, part in enumerate(pieces):
            image = bp_c[part] * z_c[part] + chunk_sum(2 + turn, k, sums)
            if not first:
                image = image + beta * q_c[part]
            q_c[part] = image
            r_c[part] = r_c[part] - alpha * image
            z_c[part] = r_c[part] / diag_c[part]
            if not final:
                gathers += gather(turn + 1, k, z_c[part])
        if not final:
            second_sweep(1 + turn, s_ref)
            observe_state()
            kept_ref[1] = kept_ref[0] - alpha[0:1] * (kept_ref[0] + y_ref[...])
        opening = lat_tile(
            event + 1, rows_tile(lon_total(event + 1, crossing), *dots((r_c, z_c), (r_c, r_c)))
        )
        if not final:
            landed(gathers)
    first_line, last_line = alphas[0][0:1], alphas[1][0:1]

    def x_step(it, carry):
        for k in range(4):
            i = it * 4 + k
            x_out[i] = first_line * r0_ref[i] + last_line * p1_ref[i]
        return carry

    stage("x_step", lax.fori_loop, 0, LAT_DEV // 4, x_step, 0)
    for j in range(own):
        spot = z * own + j
        row, col = spot // chunk, lax.rem(spot, chunk)
        start = tf[0, row, col]
        bias_out[:, j * LANES : (j + 1) * LANES] = alphas[0] * start + alphas[1] * (
            tf[1, row, col] + beta * start
        )
    totals = lat_total(2 * ITERS, opening)
    norms.append(spread(totals[0:1] + totals[2:3]))
    lane = lax.broadcasted_iota(jnp.int32, TILE, 1)
    squares = jnp.zeros(TILE, F32)
    for j in range(ITERS + 1):
        squares = jnp.where(lane == j, norms[j], squares)
    norms_out[...] = jnp.sqrt(squares)
    for copy in pending:
        copy.wait_send()
    for j in range(chunk):
        @pl.when(spots[j] // own == z)
        def _():
            sources = own_ref.at[pl.ds(0, m - 1)]
            pltpu.make_async_remote_copy(
                src_ref=sources, dst_ref=sources, send_sem=o_s.at[j], recv_sem=o_r.at[j],
                device_id=to_lon(1), device_id_type=pl.DeviceIdType.MESH,
            ).wait_send()


def publish(x_ref, bias_ref, norms_ref, x_out, bias_out, norms_out, row_ref, sems):
    row_ref[...] = norms_ref[0, : row_ref.shape[0]]
    copies = [
        pltpu.make_async_copy(src, dst, sems.at[k])
        for k, (src, dst) in enumerate(((x_ref, x_out), (bias_ref, bias_out), (row_ref, norms_out)))
    ]
    for copy in copies:
        copy.start()
    for copy in copies:
        copy.wait()


def shaped(*shape):
    return jax.ShapeDtypeStruct(shape, F32)


def body(
    innovations,
    obs_precision,
    jacobian,
    predictors,
    obs_column,
    obs_channel,
    obs_count,
    smoothing,
    bias_precision,
):
    n = lax.axis_size("swath")
    m = lax.axis_size("chan")
    owned_width = bias_precision.shape[1]
    own = owned_width // LANES
    width = own * m
    blocks = owned_width * m // CH_BLOCK
    slots = obs_precision.shape[0]
    lines = slots // OBS_BLOCK
    chunk = -(-width // n)
    parts = min(PIECES, chunk)
    half = NPRED * blocks
    grid_lines = lambda a: a.reshape(lines, OBS_BLOCK)
    held = lambda a: pltpu.with_memory_space_constraint(a, pltpu.HBM)
    vm = lambda *s: pltpu.VMEM(s, F32)
    vb = lambda *s: pltpu.VMEM(s, BF16)
    vi = lambda *s: pltpu.VMEM(s, jnp.int32)
    sem = lambda *s: pltpu.SemaphoreType.DMA(s)
    halos = 1 + ITERS
    tables = 2 + ITERS
    events = 1 + 2 * ITERS
    scratch = [
        vi(lines, OBS_BLOCK), vi(lines, OBS_BLOCK), vm(lines, OBS_BLOCK), vm(lines, OBS_BLOCK),
        vm(NPRED, slots), vb(slots, LEV),
        vb(lines, LEV, OBS_BLOCK), vb(lines // 2, CH_BLOCK, PAIR), vb(lines // 2, half, PAIR),
        vm(lines, OBS_BLOCK), vm(lines, OBS_BLOCK), vm(ITERS, lines, OBS_BLOCK), vm(lines + 1, LON_DEV, LEV),
        vi(8, LANES), pltpu.SMEM((8, LANES), jnp.int32),
        vm(1 + ITERS, LAT_DEV, LON_DEV, LEV), vm(1 + ITERS, 2, 2, LAT_DEV, LEV),
        vm(LAT_DEV, LON_DEV, LEV), vm(LAT_DEV, LON_DEV, LEV), vm(LAT_DEV, LON_DEV, LEV),
        vm(LAT_DEV, LON_DEV, LEV), vm(LAT_DEV, LON_DEV, LEV),
        vm(ITERS, lines, OBS_BLOCK), vb(LAT_DEV, LON_DEV, 2 * LEV),
        vm(2 * half, CH_BLOCK), vm(tables, n, chunk, NPRED, LANES), vb(half, 2 * CH_BLOCK),
        vm(chunk, NPRED, LANES), vm(chunk, NPRED, LANES), vm(chunk, NPRED, LANES),
        vm(chunk, NPRED, LANES), vm(chunk, NPRED, LANES), vm(chunk, NPRED, LANES), vm(own, NPRED, LANES),
        vm(halos, 2, 2, LON_DEV, LEV), vm(halos, 2, 2, LAT_DEV, LEV),
        vm(halos, 4, 8, LEV), vm(2, LON_DEV, LEV), vm(2, LAT_DEV, LEV),
        vm(tables, n, chunk, NPRED, LANES), vm(tables, m, chunk, NPRED, LANES),
        vm(ITERS, n, chunk, NPRED, LANES), vm(events, m, 8, LANES), vm(events, n, 8, LANES),
        sem(6), sem(1), sem(chunk), sem(chunk), sem(halos, 3), sem(halos, 3),
        sem(tables, parts), sem(tables, parts), sem(tables, parts), sem(tables, parts),
        sem(ITERS, parts), sem(ITERS, parts), sem(events), sem(events), sem(events), sem(events),
    ]
    VM = pl.BlockSpec(memory_space=pltpu.VMEM)
    HB = pl.BlockSpec(memory_space=pltpu.HBM)
    x, bias, norms = pl.pallas_call(
        functools.partial(kernel, n, m, own, blocks, lines, chunk),
        out_shape=(shaped(LAT_DEV, LON_DEV, LEV), shaped(NPRED, owned_width), shaped(8, LANES)),
        in_specs=[pl.BlockSpec(memory_space=pltpu.SMEM), VM, VM] + [HB] * 6,
        out_specs=(VM, VM, VM),
        scratch_shapes=scratch,
        compiler_params=pltpu.CompilerParams(
            collective_id=0, has_side_effects=True, vmem_limit_bytes=VMEM_LIMIT
        ),
        name="cg",
    )(
        obs_count, held(smoothing.reshape(1, LEV)), held(bias_precision),
        held(grid_lines(obs_column)), held(grid_lines(obs_channel)), held(grid_lines(obs_precision)),
        held(grid_lines(innovations)), held(predictors), held(jacobian),
    )
    kept = (x.shape, bias.shape, (ITERS + 1,))
    return pl.pallas_call(
        publish,
        out_shape=tuple(shaped(*shape) for shape in kept),
        in_specs=[VM, VM, VM],
        out_specs=(HB, HB, HB),
        scratch_shapes=[vm(ITERS + 1), sem(3)],
        compiler_params=pltpu.CompilerParams(vmem_limit_bytes=4 * 1024 * 1024),
        name="publish",
    )(x, bias, norms)


def solution(mesh):
    placed = (
        P(("swath", "chan")),
        P(("swath", "chan")),
        P(("swath", "chan"), None),
        P(None, ("swath", "chan")),
        P(("swath", "chan")),
        P(("swath", "chan")),
        P("swath", "chan"),
        P(),
        P(None, "chan"),
    )
    return jax.shard_map(
        body,
        mesh=mesh,
        in_specs=placed,
        out_specs=(P("swath", "chan", None), P(None, "chan"), P()),
        check_vma=False,
    )
```

```python
import functools

import jax
import jax.numpy as jnp
from jax import lax
from jax.experimental import pallas as pl
from jax.experimental.pallas import tpu as pltpu
from jax.sharding import PartitionSpec as P

LEV = 128
NPRED = 8
CH_BLOCK = 256
OBS_BLOCK = 128
LAT_DEV = 32
LON_DEV = 64
ITERS = 2
LINES = 8
PAIRS = LINES // 2
SQUARE_STEP, TABLE_STEP, LOOK_STEP, ADJOINT_STEP, FORWARD_STEP = 4, 8, 8, 4, 4
PAIR = 2 * OBS_BLOCK
LANES = 128
PIECES = 1
TILE = (8, LANES)
F32 = jnp.float32
BF16 = jnp.bfloat16
NT = (((1,), (1,)), ((), ()))
VMEM_LIMIT = 44 * 1024 * 1024


def halves(value):
    high = value.astype(BF16)
    return high, (value - high.astype(F32)).astype(BF16)


def fold(value):
    total = value[0:8]
    for i in range(1, value.shape[0] // 8):
        total = total + value[8 * i : 8 * i + 8]
    return total


def total_of(parts):
    total = parts[0]
    for part in parts[1:]:
        total = total + part
    return total


def stage(name, run, *args):
    return run(*args)


def kernel(n, m, own, blocks, lines, chunk, *refs):
    refs = list(refs)
    take = lambda k: [refs.pop(0) for _ in range(k)]
    count_ref, smooth_ref, bprec_ref = take(3)
    cell_h, chan_h, prec_h, innov_h, pred_h, jac_h = take(6)
    x_out, bias_out, norms_out = take(3)
    cell_ref, chan_ref, prec_ref, innov_ref, pred_ref, jac_ref = take(6)
    turned_ref, hot_ref, msk_ref, w_ref, y_ref, f_ref, part_ref = take(7)
    index_v, index_s = take(2)
    g_ref, gc_ref, r0_ref, r1_ref, p1_ref, q_ref, s_ref, kept_ref, split_ref = take(9)
    acc_ref, table_ref, coef_ref = take(3)
    bp_c, diag_c, r_c, p_c, z_c, q_c, own_ref = take(7)
    hv, hc, hx, rim_rows, rim_cols, ta, bb, tf, sz, sw = take(10)
    in_s, ix_s, o_s, o_r, h_s, h_r, ta_s, ta_r, b_s, b_r, c_s, c_r, z_s, z_r, w_s, w_r = take(16)
    width = own * m
    groups = lines // LINES
    me = lax.axis_index("swath")
    z = lax.axis_index("chan")
    per = CH_BLOCK // LANES
    count = min(PIECES, chunk)
    cuts = [chunk * k // count for k in range(count + 1)]
    pieces = [pl.ds(a, b - a) for a, b in zip(cuts, cuts[1:])]

    def to_lat(d):
        return {"swath": lax.rem(me + d, n)}

    def to_lon(d):
        return {"chan": lax.rem(z + d, m)}

    pending = []

    def send(src, dst, ss, rs, dev):
        copy = pltpu.make_async_remote_copy(
            src_ref=src, dst_ref=dst, send_sem=ss, recv_sem=rs,
            device_id=dev, device_id_type=pl.DeviceIdType.MESH,
        )
        copy.start()

    def sent(ref, ss, rs):
        group = pltpu.make_async_remote_copy(
            src_ref=ref, dst_ref=ref, send_sem=ss, recv_sem=rs,
            device_id=to_lon(1), device_id_type=pl.DeviceIdType.MESH,
        )
        pending.append(group)
        return group

    def await_all(copies):
        for copy in copies:
            copy.wait_recv()

    def landed(copies):
        stage("wait", await_all, copies)

    def diagonal(d, e):
        return {"swath": lax.rem(me + d, n), "chan": lax.rem(z + e, m)}

    corners = [(1, 1), (1, m - 1), (n - 1, 1), (n - 1, m - 1)]
    loads = []
    for k, (src, dst) in enumerate((
        (chan_h, chan_ref), (prec_h, prec_ref), (pred_h, pred_ref),
        (innov_h, innov_ref), (cell_h, cell_ref), (jac_h, jac_ref),
    )):
        copy = pltpu.make_async_copy(src, dst, in_s.at[k])
        copy.start()
        loads.append(copy)
    barrier = pltpu.get_barrier_semaphore()
    for d in range(1, n):
        pl.semaphore_signal(barrier, inc=1, device_id=to_lat(d), device_id_type=pl.DeviceIdType.MESH)
    for d in range(1, m):
        pl.semaphore_signal(barrier, inc=1, device_id=to_lon(d), device_id_type=pl.DeviceIdType.MESH)

    for d, e in corners:
        pl.semaphore_signal(
            barrier, inc=1, device_id=diagonal(d, e), device_id_type=pl.DeviceIdType.MESH
        )

    load_chan, load_prec, load_pred, load_innov, load_cell, load_jac = loads

    count = count_ref[0, 0]
    sub = lax.broadcasted_iota(jnp.int32, TILE, 0)
    slot8 = sub * OBS_BLOCK + lax.broadcasted_iota(jnp.int32, TILE, 1)

    def pairs_of(tile):
        return [
            jnp.concatenate([tile[2 * p : 2 * p + 1], tile[2 * p + 1 : 2 * p + 2]], axis=1)
            for p in range(PAIRS)
        ]

    def rows_of(row, count):
        packed = jnp.broadcast_to(row, (16, row.shape[1])).astype(BF16)
        return jnp.concatenate([packed] * (count // 16), axis=0)

    def stack_left(term, mask):
        high = term.astype(BF16).astype(F32)
        low = term - high
        sides = []
        for side in (high, low):
            twice = jnp.concatenate([side, side], axis=0).astype(BF16)
            sides.append(jnp.concatenate([twice] * (blocks // 2), axis=0) * mask)
        return jnp.concatenate(sides, axis=0)

    def add_table(lefts, hots):
        acc_ref[...] += lax.dot_general(
            jnp.concatenate(lefts, axis=1), jnp.concatenate(hots, axis=1), NT,
            preferred_element_type=F32,
        )

    def preds_of(it, p):
        start = pl.multiple_of((it * PAIRS + p) * PAIR, PAIR)
        return pred_ref[:, pl.ds(start, PAIR)]

    def write_table(s):
        half = NPRED * blocks
        for j in range(n * chunk):
            if j < width:
                top = (j // per) * NPRED
                lanes = slice((j % per) * LANES, (j % per + 1) * LANES)
                tile = acc_ref[top : top + NPRED, lanes] + acc_ref[half + top : half + top + NPRED, lanes]
            else:
                tile = jnp.zeros((NPRED, LANES), F32)
            table_ref[s, j // chunk, j % chunk] = tile

    def scatter(s):
        groups = []
        for k, part in enumerate(pieces):
            for d in range(1, n):
                send(
                    table_ref.at[s, lax.rem(me + d, n), part], ta.at[s, d, part],
                    ta_s.at[s, k], ta_r.at[s, k], to_lat(d),
                )
            groups.append(sent(ta.at[s, pl.ds(1, n - 1), part], ta_s.at[s, k], ta_r.at[s, k]))
        return groups

    def across(s, arriving, between=None):
        leaving = []
        for k, part in enumerate(pieces):
            if between is not None:
                between(k)
            landed([arriving[k]])
            bb[s, z, part] = total_of([table_ref[s, me, part]] + [ta[s, d, part] for d in range(1, n)])
            for d in range(1, m):
                send(bb.at[s, z, part], bb.at[s, z, part], b_s.at[s, k], b_r.at[s, k], to_lon(d))
            leaving.append(sent(bb.at[s, pl.ds(0, m - 1), part], b_s.at[s, k], b_r.at[s, k]))
        return leaving

    def chunk_sum(s, k, arriving):
        landed([arriving[k]])
        return total_of([bb[s, j, pieces[k]] for j in range(m)])

    def gather(i, k, value):
        part = pieces[k]
        tf[i, me, part] = value
        for d in range(1, n):
            send(tf.at[i, me, part], tf.at[i, me, part], c_s.at[i, k], c_r.at[i, k], to_lat(d))
        return [sent(tf.at[i, pl.ds(0, n - 1), part], c_s.at[i, k], c_r.at[i, k])]

    def lon_tile(e, tile):
        sz[e, z] = tile
        for d in range(1, m):
            send(sz.at[e, z], sz.at[e, z], z_s.at[e], z_r.at[e], to_lon(d))
        return [sent(sz.at[e, pl.ds(0, m - 1)], z_s.at[e], z_r.at[e])]

    def lon_total(e, copies):
        landed(copies)
        return total_of([sz[e, j] for j in range(m)])

    def lat_tile(e, tile):
        sw[e, me] = tile
        for d in range(1, n):
            send(sw.at[e, me], sw.at[e, me], w_s.at[e], w_r.at[e], to_lat(d))
        return [sent(sw.at[e, pl.ds(0, n - 1)], w_s.at[e], w_r.at[e])]

    def lat_total(e, copies):
        landed(copies)
        return jnp.sum(total_of([sw[e, j] for j in range(n)]), axis=1, keepdims=True)

    def rows_tile(*tiles):
        out = jnp.zeros(TILE, F32)
        for k, tile in enumerate(tiles):
            out = jnp.where(sub == k, jnp.sum(tile, axis=0, keepdims=True), out)
        return out

    def halo(k, wide):
        field, cols = g_ref.at[k], gc_ref.at[k]
        count = 2 if wide else 1
        last = pl.ds(LAT_DEV - count, count)
        near = pl.ds(0, count)
        far = pl.ds(2 - count, count)
        moves = [
            (0, field.at[last], hv.at[k, 0, far], to_lat(1)),
            (0, field.at[near], hv.at[k, 1, near], to_lat(n - 1)),
            (1, cols.at[1, far], hc.at[k, 0, far], to_lon(1)),
            (1, cols.at[0, near], hc.at[k, 1, near], to_lon(m - 1)),
        ]
        groups = [hv.at[k, pl.ds(0, 2), near], hc.at[k, pl.ds(0, 2), near]]
        if wide:
            top, end = pl.ds(0, 1), pl.ds(LAT_DEV - 1, 1)
            sources = (cols.at[1, 1, end], cols.at[0, 0, end], cols.at[1, 1, top], cols.at[0, 0, top])
            for q, (src, (d, e)) in enumerate(zip(sources, corners)):
                moves.append((2, src, hx.at[k, q, top], diagonal(d, e)))
            groups.append(hx.at[k, pl.ds(0, len(corners)), top])
        for j, src, dst, dev in moves:
            send(src, dst, h_s.at[k, j], h_r.at[k, j], dev)
        return [sent(ref, h_s.at[k, j], h_r.at[k, j]) for j, ref in enumerate(groups)]

    load_chan.wait()
    load_prec.wait()
    load_pred.wait()
    stage("load", load_innov.wait)
    acc_ref[...] = jnp.zeros_like(acc_ref)
    iota_ch = lax.broadcasted_iota(jnp.int32, (CH_BLOCK, PAIR), 0).astype(F32).astype(BF16)
    iota_b = (lax.broadcasted_iota(jnp.int32, (NPRED * blocks, PAIR), 0) // NPRED).astype(F32).astype(BF16)
    one, none = jnp.ones((), BF16), jnp.zeros((), BF16)

    def square_step(step, carry):
        lefts, hots = [], []
        for g in range(SQUARE_STEP):
            it = step * SQUARE_STEP + g
            base = pl.multiple_of(it * LINES, LINES)
            w8 = jnp.where(base * OBS_BLOCK + slot8 < count, prec_ref[pl.ds(base, LINES), :], 0.0)
            w_ref[pl.ds(base, LINES), :] = w8
            y_ref[pl.ds(base, LINES), :] = w8 * innov_ref[pl.ds(base, LINES), :]
            weights = pairs_of(w8)
            chan8 = chan_ref[pl.ds(base, LINES), :]
            lows = pairs_of((chan8 % CH_BLOCK).astype(F32))
            tops = pairs_of((chan8 // CH_BLOCK).astype(F32))
            for p in range(PAIRS):
                hot = jnp.where(iota_ch == rows_of(lows[p], CH_BLOCK), one, none)
                mask = jnp.where(iota_b == rows_of(tops[p], NPRED * blocks), one, none)
                hot_ref[it * PAIRS + p] = hot
                msk_ref[it * PAIRS + p] = mask
                preds = preds_of(it, p)
                lefts.append(stack_left(preds * preds * weights[p], mask))
                hots.append(hot)
        add_table(lefts, hots)
        return carry

    stage("squares", lax.fori_loop, 0, groups // SQUARE_STEP, square_step, 0)
    stage("write", write_table, 0)

    load_cell.wait()
    first = jnp.broadcast_to(cell_ref[:, 0:1], (lines, LANES)) // LON_DEV
    iota_l = lax.broadcasted_iota(jnp.int32, (lines, LANES), 0)
    iota_r = lax.broadcasted_iota(jnp.int32, (lines, LANES), 1)
    turned = jnp.transpose(first)
    before = jnp.where((first == turned) & (iota_l < iota_r), iota_l, -1)
    before = jnp.max(before, axis=0, keepdims=True)
    last = jnp.max(jnp.where(first == iota_r, iota_l, -1), axis=0, keepdims=True)
    index_v[0:1, :] = turned[0:1, :]
    index_v[1:2, :] = jnp.where(before < 0, lines, before)
    index_v[2:3, :] = jnp.where(last < 0, lines, last)
    load_index = pltpu.make_async_copy(index_v, index_s, ix_s.at[0])
    load_index.start()

    stage("barrier", pl.semaphore_wait, barrier, n - 1 + m - 1 + len(corners))
    squares = scatter(0)
    spots = [jnp.minimum(me * chunk + j, width - 1) for j in range(chunk)]
    for j in range(own):
        own_ref[j] = bprec_ref[:, j * LANES : (j + 1) * LANES]

    def bias_copy(j, d):
        return pltpu.make_async_remote_copy(
            src_ref=own_ref.at[lax.rem(spots[j], own)], dst_ref=bp_c.at[j], send_sem=o_s.at[j],
            recv_sem=o_r.at[j], device_id=to_lon(d), device_id_type=pl.DeviceIdType.MESH,
        )

    for j in range(chunk):
        @pl.when(spots[j] // own == z)
        def _():
            for d in range(1, m):
                bias_copy(j, d).start()
            bp_c[j] = own_ref[lax.rem(spots[j], own)]

    def adjoint_bias(s):
        acc_ref[...] = jnp.zeros_like(acc_ref)

        def table_step(step, carry):
            lefts, hots = [], []
            for g in range(TABLE_STEP):
                it = step * TABLE_STEP + g
                values = pairs_of(y_ref[pl.ds(pl.multiple_of(it * LINES, LINES), LINES), :])
                for p in range(PAIRS):
                    lefts.append(stack_left(preds_of(it, p) * values[p], msk_ref[it * PAIRS + p]))
                    hots.append(hot_ref[it * PAIRS + p])
            add_table(lefts, hots)
            return carry

        stage("table", lax.fori_loop, 0, groups // TABLE_STEP, table_step, 0)
        stage("write", write_table, s)
        return scatter(s)

    iota_col = lax.broadcasted_iota(jnp.int32, (LON_DEV, OBS_BLOCK), 0)

    def jac_of(line):
        return jac_ref[pl.ds(pl.multiple_of(line * OBS_BLOCK, OBS_BLOCK), OBS_BLOCK), :]

    def adjoint_state(k):
        def line_step(step, carry):
            outs = []
            for g in range(ADJOINT_STEP):
                base = pl.multiple_of((step * ADJOINT_STEP + g) * LINES, LINES)
                cols = cell_ref[pl.ds(base, LINES), :] % LON_DEV
                values = y_ref[pl.ds(base, LINES), :]
                for l in range(0, LINES, 2):
                    rows = []
                    for j in (l, l + 1):
                        high, low = halves(jnp.where(iota_col == cols[j : j + 1, :], values[j : j + 1, :], 0.0))
                        rows.append(jnp.concatenate([high, low], axis=1))
                    jacs = jnp.concatenate([jac_of(base + l), jac_of(base + l + 1)], axis=1)
                    both = jnp.dot(
                        jnp.concatenate(rows, axis=0), jnp.concatenate([jacs, jacs], axis=0),
                        preferred_element_type=F32,
                    )
                    outs += [both[:LON_DEV, :LEV], both[LON_DEV:, LEV:]]
            first_line = step * ADJOINT_STEP * LINES
            for l in range(ADJOINT_STEP * LINES):
                part_ref[first_line + l] = outs[l] + part_ref[index_s[1, first_line + l]]
            return carry

        stage("adjoint", lax.fori_loop, 0, groups // ADJOINT_STEP, line_step, 0)

        def row_step(i, carry):
            row = part_ref[index_s[2, i]]
            g_ref[k, i] = row
            for c in range(2):
                gc_ref[k, 0, c, pl.ds(i, 1), :] = row[c : c + 1, :]
                gc_ref[k, 1, c, pl.ds(i, 1), :] = row[LON_DEV - 2 + c : LON_DEV - 1 + c, :]
            return carry

        stage("rows", lax.fori_loop, 0, LAT_DEV, row_step, 0)
        return halo(k, k < ITERS)

    smooth = smooth_ref[0:1, :]
    top_keep = (me > 0).astype(F32)
    bottom_keep = (me < n - 1).astype(F32)
    column = lax.broadcasted_iota(jnp.int32, (LON_DEV, LEV), 0)
    zero = jnp.zeros((LON_DEV, LEV), F32)

    def relaxed(mid, above, below, left, right):
        return mid + smooth * (above + below + left + right - 4.0 * mid)

    def rim(k):
        field, cols, side = g_ref.at[k], gc_ref.at[k], hc.at[k]
        south_west, south_east, north_west, north_east = [hx[k, q, 0:1, :] for q in range(4)]
        lats = lax.broadcasted_iota(jnp.int32, (LAT_DEV, LEV), 0)

        def row(mid, above, below, west, east, keep):
            left = jnp.where(column == 0, west, pltpu.roll(mid, 1, 0))
            right = jnp.where(column == LON_DEV - 1, east, pltpu.roll(mid, LON_DEV - 1, 0))
            return relaxed(mid, above, below, left, right) * keep

        def col(mid, left, right, north, south):
            above = jnp.where(lats == 0, north * top_keep, pltpu.roll(mid, 1, 0))
            below = jnp.where(lats == LAT_DEV - 1, south * bottom_keep, pltpu.roll(mid, LAT_DEV - 1, 0))
            return relaxed(mid, above, below, left, right)

        rim_rows[0] = row(hv[k, 0, 1], hv[k, 0, 0], field[0], south_west, south_east, top_keep)
        rim_rows[1] = row(hv[k, 1, 0], field[LAT_DEV - 1], hv[k, 1, 1], north_west, north_east, bottom_keep)
        rim_cols[0] = col(side[0, 1], side[0, 0], cols[0, 0], south_west, north_west)
        rim_cols[1] = col(side[1, 0], cols[1, 1], side[1, 1], south_east, north_east)

    def sweep(field, up, down, west, east, use, acc):
        def stencil(i, above, below):
            mid = field[i]
            left = jnp.where(column == 0, west[pl.ds(i, 1), :], pltpu.roll(mid, 1, 0))
            right = jnp.where(
                column == LON_DEV - 1, east[pl.ds(i, 1), :], pltpu.roll(mid, LON_DEV - 1, 0)
            )
            return relaxed(mid, above, below, left, right)

        acc = use(0, stencil(0, up, field[1]), acc)
        inner = LAT_DEV - 2
        group = next(k for k in (5, 4, 3, 2, 1) if inner % k == 0)

        def rows(it, a):
            for k in range(group):
                i = 1 + it * group + k
                a = use(i, stencil(i, field[i - 1], field[i + 1]), a)
            return a

        acc = lax.fori_loop(0, inner // group, rows, acc)
        end = LAT_DEV - 1
        return use(end, stencil(end, field[end - 1], down), acc)

    def first_sweep(k, use):
        return fold(stage(
            "sweep", sweep, g_ref.at[k], hv[k, 0, 1] * top_keep, hv[k, 1, 0] * bottom_keep,
            hc.at[k, 0, 1], hc.at[k, 1, 0], use, zero,
        ))

    def second_sweep(k, field):
        def use(i, row, acc):
            high, low = halves(row)
            split_ref[i] = jnp.concatenate([high, low], axis=1)
            return acc

        rim(k)
        stage(
            "sweep_u", sweep, field, rim_rows[0], rim_rows[1], rim_cols.at[0], rim_cols.at[1], use, 0
        )

    def observe_state():
        def line_step(step, carry):
            for g in range(FORWARD_STEP):
                base = pl.multiple_of((step * FORWARD_STEP + g) * LINES, LINES)
                cols = cell_ref[pl.ds(base, LINES), :] % LON_DEV
                seen = []
                for l in range(0, LINES, 2):
                    fields = [split_ref[index_s[0, base + j]] for j in (l, l + 1)]
                    jacs = jnp.concatenate([turned_ref[base + l], turned_ref[base + l + 1]], axis=1)
                    both = jnp.dot(
                        jnp.concatenate(fields, axis=0), jnp.concatenate([jacs, jacs], axis=0),
                        preferred_element_type=F32,
                    )
                    for j, part in ((l, both[:LON_DEV, :OBS_BLOCK]), (l + 1, both[LON_DEV:, OBS_BLOCK:])):
                        picked = jnp.where(iota_col == cols[j : j + 1, :], part, 0.0)
                        seen.append(jnp.sum(picked, axis=0, keepdims=True))
                y_ref[pl.ds(base, LINES), :] = jnp.concatenate(seen, axis=0)
            return carry

        stage("forward", lax.fori_loop, 0, groups // FORWARD_STEP, line_step, 0)

    def forward_bias(i):
        for b in range(blocks):
            for h in range(per):
                j = b * per + h
                high, low = halves(tf[i, j // chunk, j % chunk])
                coef_ref[b * NPRED : (b + 1) * NPRED, h * LANES : (h + 1) * LANES] = high
                coef_ref[b * NPRED : (b + 1) * NPRED, CH_BLOCK + h * LANES : CH_BLOCK + (h + 1) * LANES] = low
        coef2 = coef_ref[...]

        def look_step(step, acc):
            for g in range(LOOK_STEP):
                it = step * LOOK_STEP + g
                base = pl.multiple_of(it * LINES, LINES)
                tops = pairs_of(chan_ref[pl.ds(base, LINES), :] // CH_BLOCK)
                looked = []
                for p in range(PAIRS):
                    hot = hot_ref[it * PAIRS + p]
                    mid = jnp.dot(coef2, jnp.concatenate([hot, hot], axis=0), preferred_element_type=F32)
                    which = jnp.broadcast_to(tops[p], (NPRED, PAIR))
                    total = jnp.zeros((NPRED, PAIR), F32)
                    for b in range(blocks):
                        total = jnp.where(which == b, mid[b * NPRED : (b + 1) * NPRED], total)
                    total = jnp.sum(total * preds_of(it, p), axis=0, keepdims=True)
                    looked += [total[:, :OBS_BLOCK], total[:, OBS_BLOCK:]]
                f8 = kept_ref[i, pl.ds(base, LINES), :] + jnp.concatenate(looked, axis=0)
                y8 = w_ref[pl.ds(base, LINES), :] * f8
                f_ref[i, pl.ds(base, LINES), :] = f8
                y_ref[pl.ds(base, LINES), :] = y8
                acc = acc + y8 * f8
            return acc

        return stage("look", lax.fori_loop, 0, groups // LOOK_STEP, look_step, jnp.zeros(TILE, F32))

    def spread(column):
        return jnp.broadcast_to(column, TILE)

    def dots(*pairs):
        return [total_of([a[j] * b[j] for j in range(chunk)]) for a, b in pairs]

    part_ref[lines] = zero
    sums = adjoint_bias(1)
    load_index.wait()
    stage("load_jac", load_jac.wait)
    halos = adjoint_state(0)
    squares = across(0, squares)

    def turn_step(it, carry):
        for l in range(LINES):
            turned_ref[it * LINES + l] = jnp.transpose(jac_of(it * LINES + l))
        return carry

    turns = [groups * k // len(pieces) for k in range(len(pieces) + 1)]

    def turn_some(k):
        stage("turn", lax.fori_loop, turns[k], turns[k + 1], turn_step, 0)

    sums = across(1, sums, turn_some)
    landed(halos)

    def use_first(i, row, acc):
        r0_ref[i] = row
        return acc + row * row

    pp_state = first_sweep(0, use_first)
    crossing = lon_tile(0, pp_state)
    second_sweep(0, r0_ref)
    for j in range(chunk):
        @pl.when(spots[j] // own != z)
        def _():
            bias_copy(j, 1).wait_recv()

    gathers = []
    for k, part in enumerate(pieces):
        diag_c[part] = bp_c[part] + chunk_sum(0, k, squares)
        r_c[part] = chunk_sum(1, k, sums)
        z_c[part] = r_c[part] / diag_c[part]
        p_c[part] = z_c[part]
        gathers += gather(0, k, z_c[part])
    observe_state()
    kept_ref[0] = y_ref[...]
    opening = lat_tile(0, rows_tile(lon_total(0, crossing), *dots((r_c, p_c), (r_c, r_c))))
    landed(gathers)
    alphas, norms = [], []
    beta = None
    for turn in range(ITERS):
        first, final = turn == 0, turn == ITERS - 1
        event = 1 + 2 * turn
        observed = forward_bias(turn)
        totals = lat_total(event - 1, opening)
        new = spread(totals[0:1] + totals[1:2])
        norms.append(spread(totals[0:1] + totals[2:3]))
        if not first:
            beta = new / rz
            slope = beta[0:1]

            def p_step(it, acc):
                for k in range(4):
                    i = it * 4 + k
                    row = r1_ref[i] + slope * r0_ref[i]
                    p1_ref[i] = row
                    acc = acc + row * row
                return acc

            pp_state = fold(stage("p_step", lax.fori_loop, 0, LAT_DEV // 4, p_step, zero))
            joined = f_ref[turn] + slope * f_ref[turn - 1]
            observed = fold(w_ref[...] * joined * joined)
            p_c[...] = z_c[...] + beta * p_c[...]
        rz = new
        crossing = lon_tile(event, pp_state + observed)
        sums = adjoint_bias(2 + turn)
        pp_bias = total_of([bp_c[j] * p_c[j] * p_c[j] for j in range(chunk)])
        around = lat_tile(event, rows_tile(lon_total(event, crossing), pp_bias))
        halos = adjoint_state(1 + turn)
        sums = across(2 + turn, sums)
        totals = lat_total(event, around)
        alpha = rz / spread(totals[0:1] + totals[1:2])
        alphas.append(alpha)
        line = alpha[0:1]
        landed(halos)
        old_ref = r0_ref if first else r1_ref

        def use_next(i, row, acc):
            image = old_ref[i] + row
            if first:
                q_ref[i] = image
                s_ref[i] = row
            else:
                image = image + slope * q_ref[i]
            residual = old_ref[i] - line * image
            if not final:
                r1_ref[i] = residual
            return acc + residual * residual

        crossing = lon_tile(event + 1, first_sweep(1 + turn, use_next))
        gathers = []
        for k, part in enumerate(pieces):
            image = bp_c[part] * z_c[part] + chunk_sum(2 + turn, k, sums)
            if not first:
                image = image + beta * q_c[part]
            q_c[part] = image
            r_c[part] = r_c[part] - alpha * image
            z_c[part] = r_c[part] / diag_c[part]
            if not final:
                gathers += gather(turn + 1, k, z_c[part])
        if not final:
            second_sweep(1 + turn, s_ref)
            observe_state()
            kept_ref[1] = kept_ref[0] - alpha[0:1] * (kept_ref[0] + y_ref[...])
        opening = lat_tile(
            event + 1, rows_tile(lon_total(event + 1, crossing), *dots((r_c, z_c), (r_c, r_c)))
        )
        if not final:
            landed(gathers)
    first_line, last_line = alphas[0][0:1], alphas[1][0:1]

    def x_step(it, carry):
        for k in range(4):
            i = it * 4 + k
            x_out[i] = first_line * r0_ref[i] + last_line * p1_ref[i]
        return carry

    stage("x_step", lax.fori_loop, 0, LAT_DEV // 4, x_step, 0)
    for j in range(own):
        spot = z * own + j
        row, col = spot // chunk, lax.rem(spot, chunk)
        start = tf[0, row, col]
        bias_out[:, j * LANES : (j + 1) * LANES] = alphas[0] * start + alphas[1] * (
            tf[1, row, col] + beta * start
        )
    while len(pending) > 1:
        pending.pop(0).wait_send()
    for j in range(chunk):
        @pl.when(spots[j] // own == z)
        def _():
            sources = own_ref.at[pl.ds(0, m - 1)]
            pltpu.make_async_remote_copy(
                src_ref=sources, dst_ref=sources, send_sem=o_s.at[j], recv_sem=o_r.at[j],
                device_id=to_lon(1), device_id_type=pl.DeviceIdType.MESH,
            ).wait_send()
    totals = lat_total(2 * ITERS, opening)
    norms.append(spread(totals[0:1] + totals[2:3]))
    lane = lax.broadcasted_iota(jnp.int32, TILE, 1)
    squares = jnp.zeros(TILE, F32)
    for j in range(ITERS + 1):
        squares = jnp.where(lane == j, norms[j], squares)
    norms_out[...] = jnp.sqrt(squares)
    pending.pop().wait_send()


def publish(x_ref, bias_ref, norms_ref, x_out, bias_out, norms_out, row_ref, sems):
    row_ref[...] = norms_ref[0, : row_ref.shape[0]]
    copies = [
        pltpu.make_async_copy(src, dst, sems.at[k])
        for k, (src, dst) in enumerate(((x_ref, x_out), (bias_ref, bias_out), (row_ref, norms_out)))
    ]
    for copy in copies:
        copy.start()
    for copy in copies:
        copy.wait()


def shaped(*shape):
    return jax.ShapeDtypeStruct(shape, F32)


def body(
    innovations,
    obs_precision,
    jacobian,
    predictors,
    obs_column,
    obs_channel,
    obs_count,
    smoothing,
    bias_precision,
):
    n = lax.axis_size("swath")
    m = lax.axis_size("chan")
    owned_width = bias_precision.shape[1]
    own = owned_width // LANES
    width = own * m
    blocks = owned_width * m // CH_BLOCK
    slots = obs_precision.shape[0]
    lines = slots // OBS_BLOCK
    chunk = -(-width // n)
    parts = min(PIECES, chunk)
    half = NPRED * blocks
    grid_lines = lambda a: a.reshape(lines, OBS_BLOCK)
    held = lambda a: pltpu.with_memory_space_constraint(a, pltpu.HBM)
    vm = lambda *s: pltpu.VMEM(s, F32)
    vb = lambda *s: pltpu.VMEM(s, BF16)
    vi = lambda *s: pltpu.VMEM(s, jnp.int32)
    sem = lambda *s: pltpu.SemaphoreType.DMA(s)
    halos = 1 + ITERS
    tables = 2 + ITERS
    events = 1 + 2 * ITERS
    scratch = [
        vi(lines, OBS_BLOCK), vi(lines, OBS_BLOCK), vm(lines, OBS_BLOCK), vm(lines, OBS_BLOCK),
        vm(NPRED, slots), vb(slots, LEV),
        vb(lines, LEV, OBS_BLOCK), vb(lines // 2, CH_BLOCK, PAIR), vb(lines // 2, half, PAIR),
        vm(lines, OBS_BLOCK), vm(lines, OBS_BLOCK), vm(ITERS, lines, OBS_BLOCK), vm(lines + 1, LON_DEV, LEV),
        vi(8, LANES), pltpu.SMEM((8, LANES), jnp.int32),
        vm(1 + ITERS, LAT_DEV, LON_DEV, LEV), vm(1 + ITERS, 2, 2, LAT_DEV, LEV),
        vm(LAT_DEV, LON_DEV, LEV), vm(LAT_DEV, LON_DEV, LEV), vm(LAT_DEV, LON_DEV, LEV),
        vm(LAT_DEV, LON_DEV, LEV), vm(LAT_DEV, LON_DEV, LEV),
        vm(ITERS, lines, OBS_BLOCK), vb(LAT_DEV, LON_DEV, 2 * LEV),
        vm(2 * half, CH_BLOCK), vm(tables, n, chunk, NPRED, LANES), vb(half, 2 * CH_BLOCK),
        vm(chunk, NPRED, LANES), vm(chunk, NPRED, LANES), vm(chunk, NPRED, LANES),
        vm(chunk, NPRED, LANES), vm(chunk, NPRED, LANES), vm(chunk, NPRED, LANES), vm(own, NPRED, LANES),
        vm(halos, 2, 2, LON_DEV, LEV), vm(halos, 2, 2, LAT_DEV, LEV),
        vm(halos, 4, 8, LEV), vm(2, LON_DEV, LEV), vm(2, LAT_DEV, LEV),
        vm(tables, n, chunk, NPRED, LANES), vm(tables, m, chunk, NPRED, LANES),
        vm(ITERS, n, chunk, NPRED, LANES), vm(events, m, 8, LANES), vm(events, n, 8, LANES),
        sem(6), sem(1), sem(chunk), sem(chunk), sem(halos, 3), sem(halos, 3),
        sem(tables, parts), sem(tables, parts), sem(tables, parts), sem(tables, parts),
        sem(ITERS, parts), sem(ITERS, parts), sem(events), sem(events), sem(events), sem(events),
    ]
    VM = pl.BlockSpec(memory_space=pltpu.VMEM)
    HB = pl.BlockSpec(memory_space=pltpu.HBM)
    x, bias, norms = pl.pallas_call(
        functools.partial(kernel, n, m, own, blocks, lines, chunk),
        out_shape=(shaped(LAT_DEV, LON_DEV, LEV), shaped(NPRED, owned_width), shaped(8, LANES)),
        in_specs=[pl.BlockSpec(memory_space=pltpu.SMEM), VM, VM] + [HB] * 6,
        out_specs=(VM, VM, VM),
        scratch_shapes=scratch,
        compiler_params=pltpu.CompilerParams(
            collective_id=0, has_side_effects=True, vmem_limit_bytes=VMEM_LIMIT
        ),
        name="cg",
    )(
        obs_count, held(smoothing.reshape(1, LEV)), held(bias_precision),
        held(grid_lines(obs_column)), held(grid_lines(obs_channel)), held(grid_lines(obs_precision)),
        held(grid_lines(innovations)), held(predictors), held(jacobian),
    )
    kept = (x.shape, bias.shape, (ITERS + 1,))
    return pl.pallas_call(
        publish,
        out_shape=tuple(shaped(*shape) for shape in kept),
        in_specs=[VM, VM, VM],
        out_specs=(HB, HB, HB),
        scratch_shapes=[vm(ITERS + 1), sem(3)],
        compiler_params=pltpu.CompilerParams(vmem_limit_bytes=4 * 1024 * 1024),
        name="publish",
    )(x, bias, norms)


def solution(mesh):
    placed = (
        P(("swath", "chan")),
        P(("swath", "chan")),
        P(("swath", "chan"), None),
        P(None, ("swath", "chan")),
        P(("swath", "chan")),
        P(("swath", "chan")),
        P("swath", "chan"),
        P(),
        P(None, "chan"),
    )
    return jax.shard_map(
        body,
        mesh=mesh,
        in_specs=placed,
        out_specs=(P("swath", "chan", None), P(None, "chan"), P()),
        check_vma=False,
    )
```
